256 devices in a mesh: pair: 32 (over x, z_hi, core), aux: 8 (over z_lo, y).
Axes of the slice: x: 4, y: 4, z: 8 (z_hi: 4, z_lo: 2; z = z_hi * 2 + z_lo), core: 2. Of those that a mesh axis runs over, the one named last changes fastest.
Arguments:
- integrals: float32 [32, 640, 4096], P(None, 'aux', 'pair'), may hold values from -6 to 6
- factor: float32 [4096, 4096], P('aux', 'pair'), may hold values from -1 to 2, as said below
- diag_inverse: float32 [8, 512, 512], P('aux'), may hold values from -1 to 1, as said below
Outputs:
- transformed: float32 [32, 640, 4096], P('pair', None, 'aux')
The draws below stay inside these ranges and needn't reach their ends.
Inputs may be any that keep to these rules, and one draw needn't show every extreme that they name: factor is zero above its diagonal. diag_inverse[j] is the inverse, up to rounding, of the factor's j-th diagonal block of 512 x 512.
All inputs are finite; a program needn't handle non-finite values.
Results may differ from the reference program's by a relative error of at most 0.0001.
Values sent between devices are 32-bit elements; how exact they have to be, the bound alone decides.
No kernel may reach another device: no remote copies, remote signals or barrier semaphores. Data moves between devices by JAX's collectives and lax.ppermute only.
A program may use at most 128 MiB of HBM per device.

```python
import math
import jax
import jax.numpy as jnp
from jax import lax

PANEL = 512
VIRT = 640
OCC = 32
WIN = 4096


def factor_parts(key):
    base = jax.random.fold_in(key, 7)
    first, second = jax.random.split(base)
    diagonal = jax.random.uniform(first, (WIN,), jnp.float32, 1.0, 2.0)
    below = jnp.clip(jax.random.normal(second, (WIN, WIN), jnp.float32), -6.0, 6.0)
    below = below * (0.6 / math.sqrt(WIN))
    factor = jnp.tril(below, -1) + jnp.diag(diagonal)
    blocks = jnp.stack([factor[j * PANEL:(j + 1) * PANEL, j * PANEL:(j + 1) * PANEL] for j in range(WIN // PANEL)])
    identity = jnp.broadcast_to(jnp.eye(PANEL, dtype=jnp.float32), blocks.shape)
    inverses = lax.linalg.triangular_solve(blocks, identity, left_side=True, lower=True)
    return (factor, inverses)


def draw_factor(key, part):
    return factor_parts(key)[0]


def draw_diag_inverse(key, part):
    return factor_parts(key)[1]


def shard_levels(own_key, dims, cuts, least, high):
    loudness = 1.0
    for position, shards_of in cuts:
        draws = jax.random.uniform(jax.random.fold_in(jax.random.fold_in(own_key, 6), position), (shards_of,), jnp.float32, least / len(cuts), high / len(cuts))
        loudness = loudness * jnp.repeat(jnp.exp(draws), dims[position] // shards_of).reshape((-1,) + (1,) * (len(dims) - 1 - position))
    return loudness


def gaussian(own_key, extent, width, limit, pieces=(), kind=jnp.bfloat16):
    result = width * jax.random.normal(own_key, extent, jnp.float32)
    if pieces:
        result = result * shard_levels(own_key, extent, pieces, -0.22, 0.18)
    return jnp.clip(result, -limit, limit).astype(kind)


def setup_inputs(seed: int = 0) -> dict:
    streams_of = jax.random.split(jax.random.key(seed), 4)
    integrals = gaussian(streams_of[0], (OCC, VIRT, WIN), 1.0, 6.0, ((1, 8), (2, 32)), jnp.float32)
    factor = draw_factor(jax.random.fold_in(streams_of[3], 71), 0)
    diag_inverse = draw_diag_inverse(jax.random.fold_in(streams_of[3], 71), 0)
    return dict(integrals=integrals, factor=factor, diag_inverse=diag_inverse)


def reference(integrals, factor, diag_inverse):
    pair_rows = integrals.reshape(-1, WIN)
    panel_count = WIN // PANEL
    solved = []
    for step in range(panel_count):
        remain = pair_rows[:, step * PANEL:(step + 1) * PANEL]
        if step > 0:
            earlier = jnp.concatenate(solved, axis=1)
            factor_block = factor[step * PANEL:(step + 1) * PANEL, :step * PANEL]
            remain = remain - jnp.dot(earlier.astype(jnp.float32), factor_block.T.astype(jnp.float32), precision=lax.Precision.HIGHEST, preferred_element_type=jnp.float32)
        solved.append(jnp.dot(remain.astype(jnp.float32), diag_inverse[step].T.astype(jnp.float32), precision=lax.Precision.HIGHEST, preferred_element_type=jnp.float32))
    return jnp.concatenate(solved, axis=1).reshape(OCC, VIRT, WIN)
```

```python
import functools
import jax
import jax.numpy as jnp
from jax import lax
from jax.experimental import pallas as pl
from jax.experimental.pallas import tpu as pltpu
from jax.sharding import PartitionSpec as P

NX, NY, NZ = 4, 4, 8
ALL = ("pair", "aux")
EARLY, LATE = 5, 4
SLOTS = EARLY + LATE
PANELS, PANEL, LANES, ROWS = 8, 512, 128, 80
STEPS = (0, -1, 1, 2)


def device_id(x, y, z, core):
    return ((x * NZ // 2 + z // 2) * 2 + core) * 8 + (z % 2) * NY + y


def shift(value, dx=0, dy=0, dz=0, core=0):
    pairs = [
        (device_id(x, y, z, c), device_id((x + dx) % NX, (y + dy) % NY, (z + dz) % NZ, (c + core) % 2))
        for x in range(NX)
        for y in range(NY)
        for z in range(NZ)
        for c in range(2)
    ]
    return lax.ppermute(value, ALL, pairs)


def along(axis):
    return lambda value, d: shift(value, **{axis: d})


def rings(block, first, second):
    one, two = along(first), along(second)
    up, down = one(block, 1), one(block, -1)
    far = jnp.concatenate([one(up[:4], 1), one(down[4:], -1)])
    whole = jnp.stack([block, up, down, far])
    up, down = two(whole, 1), two(whole, -1)
    far_up, far_down = two(up[:2], 1), two(down[2:], -1)
    return [whole, up, down, far_up, far_down]


def pieces(factor, diag_inverse, pair, aux):
    column = pair // 4
    diagonal = lax.dynamic_slice(diag_inverse[0], (0, LANES * (pair % 4)), (PANEL, LANES))
    slab = jnp.where(column == aux, diagonal, factor)
    chunks = slab.reshape(2, 8, 32, LANES).transpose(1, 0, 2, 3)
    chunks = lax.all_to_all(chunks, "aux", 0, 0, tiled=True)
    own = chunks[:, 0]
    other = lax.ppermute(chunks[:, 1], "pair", [(p, 31 - p) for p in range(32)])
    is_low = column < 4
    low = jnp.where(is_low, own, other)
    high = jnp.where(is_low, other, own)
    both = jnp.concatenate([low, high])
    least = jnp.minimum(column, 7 - column)
    held = []
    for slot in range(SLOTS):
        paired = (slot + 7) // 2 if slot % 2 else 8 + (slot + 6) // 2
        index = jnp.where(slot < 7 - 2 * least, slot + least, paired)
        held.append(lax.dynamic_index_in_dim(both, index, 0, keepdims=False))
    return jnp.stack(held)


def kernel(*refs):
    place_ref, x_ref = refs[:2]
    arrays = refs[2:22]
    out_ref, held, remain, parts, early_sem, late_sem = refs[22:]
    x, y, z, core = (place_ref[i] for i in range(4))

    def fetch(sources, dx, dy, from_core, first_slot, sem):
        sx, sy = lax.rem(x + dx + NX, NX), lax.rem(y + dy + NY, NY)

        @pl.loop(0, NZ)
        def _(dz):
            sz = lax.rem(z - dz + NZ, NZ)
            holder = sx * 8 + lax.div(sz, 2) * 2 + from_core
            group = lax.rem(sz, 2) * NY + sy
            count = sources.shape[1]
            pltpu.make_async_copy(
                sources.at[dz], held.at[holder, pl.ds(first_slot, count), group], sem
            ).start()

    def fetch_all(five, from_core, first_slot, sem, order):
        for number, (ref, second, blocks) in enumerate(
            zip(five, (0, -1, 1, -2, 2), ((0, 1, 2, 3),) * 3 + ((0, 1), (2, 3)), strict=True)
        ):
            for at, block in enumerate(blocks):
                first = STEPS[block]
                dx, dy = (first, second) if order == "xy" else (second, first)
                fetch(ref.at[at], dx, dy, from_core, first_slot, sem)

    fetch_all(arrays[0:5], core, 0, early_sem, "xy")
    fetch_all(arrays[5:10], 1 - core, 0, early_sem, "xy")
    fetch_all(arrays[10:15], core, EARLY, late_sem, "yx")
    fetch_all(arrays[15:20], 1 - core, EARLY, late_sem, "yx")

    def product(left, j, k):
        low_slot = jnp.where(j < 7 - k, j - k, 2 * j - 7)
        slot = jnp.where(k < 4, low_slot, 2 * j - 6)
        halves = []
        for half in range(2):
            total = None
            for pair in range(2):
                tiles = []
                for s in range(2):
                    p = 4 * k + 2 * pair + s
                    holder = 31 - p if half else p
                    tiles.append(held[holder, slot].reshape(256, LANES))
                weight = jnp.concatenate(tiles, axis=1)
                high = weight.astype(jnp.bfloat16)
                low = (weight - high.astype(jnp.float32)).astype(jnp.bfloat16)
                part = left[:, 256 * pair : 256 * (pair + 1)]
                dims = (((1,), (1,)), ((), ()))
                twice = lax.dot_general(part, high, dims, preferred_element_type=jnp.float32)
                once = lax.dot_general(part[:ROWS], low, dims, preferred_element_type=jnp.float32)
                piece = twice[:ROWS] + (twice[ROWS:] + once)
                total = piece if total is None else total + piece
            halves.append(total)
        return jnp.concatenate(halves, axis=1)

    def split(value):
        high = value.astype(jnp.bfloat16)
        low = (value - high.astype(jnp.float32)).astype(jnp.bfloat16)
        return jnp.concatenate([high, low], axis=0)

    def panel(j, carry):
        remain[...] = jnp.concatenate([x_ref[4 * j + s] for s in range(4)], axis=1)

        def update(k, carry):
            remain[...] -= product(parts[k], j, k)
            return carry

        lax.fori_loop(0, j, update, 0)
        solved = product(split(remain[...]), j, j)
        out_ref[j] = solved
        parts[j] = split(solved)
        return carry

    early = held.at[:, pl.ds(0, EARLY)]
    pltpu.make_async_copy(early, early, early_sem).wait()
    lax.fori_loop(0, EARLY, panel, 0)
    late = held.at[:, pl.ds(EARLY, LATE)]
    pltpu.make_async_copy(late, late, late_sem).wait()
    lax.fori_loop(EARLY, PANELS, panel, 0)


def solve(place, rows, arrays):
    return pl.pallas_call(
        kernel,
        out_shape=jax.ShapeDtypeStruct((PANELS, ROWS, PANEL), jnp.float32),
        in_specs=[pl.BlockSpec(memory_space=pltpu.SMEM), pl.BlockSpec(memory_space=pltpu.VMEM)]
        + [pl.BlockSpec(memory_space=pltpu.HBM)] * len(arrays),
        out_specs=pl.BlockSpec(memory_space=pltpu.VMEM),
        scratch_shapes=[
            pltpu.VMEM((32, SLOTS, 8, 32, LANES), jnp.float32),
            pltpu.VMEM((ROWS, PANEL), jnp.float32),
            pltpu.VMEM((PANELS, 2 * ROWS, PANEL), jnp.bfloat16),
            pltpu.SemaphoreType.DMA,
            pltpu.SemaphoreType.DMA,
        ],
        compiler_params=pltpu.CompilerParams(vmem_limit_bytes=48 * 2**20),
        cost_estimate=pl.CostEstimate(flops=16 * 10**9, bytes_accessed=40 * 10**6, transcendentals=0),
    )(place, rows, *arrays)


def local(integrals, factor, diag_inverse):
    pair, aux = lax.axis_index("pair"), lax.axis_index("aux")
    x, z, core = pair // 8, (pair // 2) % 4 * 2 + aux // NY, pair % 2
    place = jnp.stack([x, aux % NY, z, core]).astype(jnp.int32)

    piece = pieces(factor, diag_inverse, pair, aux)
    column = jnp.stack([piece] + [shift(piece, dz=d) for d in range(1, NZ)])
    early = rings(column[:, :EARLY], "dx", "dy")
    late = rings(column[:, EARLY:], "dy", "dx")
    rows = lax.all_to_all(integrals, "pair", 0, 0, tiled=True)
    arrays = early + [shift(v, core=1) for v in early] + late + [shift(v, core=1) for v in late]
    solved = solve(place, rows, arrays)
    result = lax.all_to_all(solved, "aux", 0, 0, tiled=True)
    return result.reshape(1, 8 * ROWS, PANEL)


def solution(mesh):
    in_specs = (P(None, "aux", "pair"), P("aux", "pair"), P("aux", None, None))
    out_specs = P("pair", None, "aux")
    return jax.shard_map(local, mesh=mesh, in_specs=in_specs, out_specs=out_specs, check_vma=False)
```

```python
import functools
import jax
import jax.numpy as jnp
from jax import lax
from jax.experimental import pallas as pl
from jax.experimental.pallas import tpu as pltpu
from jax.sharding import PartitionSpec as P

NX, NY, NZ = 4, 4, 8
ALL = ("pair", "aux")
EARLY, LATE = 5, 4
SLOTS = EARLY + LATE
PANELS, PANEL, LANES, ROWS = 8, 512, 128, 80
STEPS = (0, -1, 1, 2)


def device_id(x, y, z, core):
    return ((x * NZ // 2 + z // 2) * 2 + core) * 8 + (z % 2) * NY + y


def shift(value, dx=0, dy=0, dz=0, core=0):
    pairs = [
        (device_id(x, y, z, c), device_id((x + dx) % NX, (y + dy) % NY, (z + dz) % NZ, (c + core) % 2))
        for x in range(NX)
        for y in range(NY)
        for z in range(NZ)
        for c in range(2)
    ]
    return lax.ppermute(value, ALL, pairs)


def along(axis):
    return lambda value, d: shift(value, **{axis: d})


def ring_of_eight(piece):
    up, down = [piece], [piece]
    for _ in range(3):
        up.append(shift(up[-1], dz=1))
        down.append(shift(down[-1], dz=-1))
    far = jnp.concatenate([shift(up[3][:EARLY], dz=1), shift(down[3][EARLY:], dz=-1)])
    return jnp.stack(up + [far] + down[:0:-1])


def gather(column, integrals):
    blocks = [column[:, :EARLY], column[:, EARLY:]]
    first = [along("dx"), along("dy")]
    second = [along("dy"), along("dx")]
    near = [(one(block, 1), one(block, -1)) for one, block in zip(first, blocks)]
    near = lax.optimization_barrier(near)
    far = [(one(up[:4], 1), one(down[4:], -1)) for one, (up, down) in zip(first, near)]
    whole = [
        jnp.stack([block, up, down, jnp.concatenate(ends)])
        for block, (up, down), ends in zip(blocks, near, far)
    ]
    whole, integrals = lax.optimization_barrier((whole, integrals))
    near = [(two(block, 1), two(block, -1)) for two, block in zip(second, whole)]
    rows = lax.all_to_all(integrals, "pair", 0, 0, tiled=True)
    near, rows = lax.optimization_barrier((near, rows))
    far = [(two(up[:2], 1), two(down[2:], -1)) for two, (up, down) in zip(second, near)]
    return rows, [[block, *sides, *ends] for block, sides, ends in zip(whole, near, far)]


def pieces(factor, diag_inverse, pair, aux):
    column = pair // 4
    diagonal = lax.dynamic_slice(diag_inverse[0], (0, LANES * (pair % 4)), (PANEL, LANES))
    slab = jnp.where(column == aux, diagonal, factor)
    chunks = slab.reshape(2, 8, 32, LANES).transpose(1, 0, 2, 3)
    chunks = lax.all_to_all(chunks, "aux", 0, 0, tiled=True)
    own = chunks[:, 0]
    other = lax.ppermute(chunks[:, 1], "pair", [(p, 31 - p) for p in range(32)])
    is_low = column < 4
    low = jnp.where(is_low, own, other)
    high = jnp.where(is_low, other, own)
    both = jnp.concatenate([low, high])
    least = jnp.minimum(column, 7 - column)
    held = []
    for slot in range(SLOTS):
        paired = (slot + 7) // 2 if slot % 2 else 8 + (slot + 6) // 2
        index = jnp.where(slot < 7 - 2 * least, slot + least, paired)
        held.append(lax.dynamic_index_in_dim(both, index, 0, keepdims=False))
    return jnp.stack(held)


def kernel(*refs):
    place_ref, x_ref = refs[:2]
    arrays = refs[2:22]
    out_ref, held, remain, parts, early_sem, late_sem = refs[22:]
    x, y, z, core = (place_ref[i] for i in range(4))

    def fetch(sources, dx, dy, from_core, first_slot, sem):
        sx, sy = lax.rem(x + dx + NX, NX), lax.rem(y + dy + NY, NY)

        @pl.loop(0, NZ)
        def _(dz):
            sz = lax.rem(z - dz + NZ, NZ)
            holder = sx * 8 + lax.div(sz, 2) * 2 + from_core
            group = lax.rem(sz, 2) * NY + sy
            count = sources.shape[1]
            pltpu.make_async_copy(
                sources.at[dz], held.at[holder, pl.ds(first_slot, count), group], sem
            ).start()

    def fetch_all(five, from_core, first_slot, sem, order):
        for number, (ref, second, blocks) in enumerate(
            zip(five, (0, -1, 1, -2, 2), ((0, 1, 2, 3),) * 3 + ((0, 1), (2, 3)), strict=True)
        ):
            for at, block in enumerate(blocks):
                first = STEPS[block]
                dx, dy = (first, second) if order == "xy" else (second, first)
                fetch(ref.at[at], dx, dy, from_core, first_slot, sem)

    fetch_all(arrays[0:5], core, 0, early_sem, "xy")
    fetch_all(arrays[5:10], 1 - core, 0, early_sem, "xy")
    fetch_all(arrays[10:15], core, EARLY, late_sem, "yx")
    fetch_all(arrays[15:20], 1 - core, EARLY, late_sem, "yx")

    def product(left, j, k):
        low_slot = jnp.where(j < 7 - k, j - k, 2 * j - 7)
        slot = jnp.where(k < 4, low_slot, 2 * j - 6)
        halves = []
        for half in range(2):
            total = None
            for pair in range(2):
                tiles = []
                for s in range(2):
                    p = 4 * k + 2 * pair + s
                    holder = 31 - p if half else p
                    tiles.append(held[holder, slot].reshape(256, LANES))
                weight = jnp.concatenate(tiles, axis=1)
                high = weight.astype(jnp.bfloat16)
                low = (weight - high.astype(jnp.float32)).astype(jnp.bfloat16)
                part = left[:, 256 * pair : 256 * (pair + 1)]
                dims = (((1,), (1,)), ((), ()))
                twice = lax.dot_general(part, high, dims, preferred_element_type=jnp.float32)
                once = lax.dot_general(part[:ROWS], low, dims, preferred_element_type=jnp.float32)
                piece = twice[:ROWS] + (twice[ROWS:] + once)
                total = piece if total is None else total + piece
            halves.append(total)
        return jnp.concatenate(halves, axis=1)

    def split(value):
        high = value.astype(jnp.bfloat16)
        low = (value - high.astype(jnp.float32)).astype(jnp.bfloat16)
        return jnp.concatenate([high, low], axis=0)

    def panel(j, carry):
        remain[...] = jnp.concatenate([x_ref[4 * j + s] for s in range(4)], axis=1)

        def update(k, carry):
            remain[...] -= product(parts[k], j, k)
            return carry

        lax.fori_loop(0, j, update, 0)
        solved = product(split(remain[...]), j, j)
        out_ref[j] = solved
        parts[j] = split(solved)
        return carry

    early = held.at[:, pl.ds(0, EARLY)]
    pltpu.make_async_copy(early, early, early_sem).wait()
    lax.fori_loop(0, EARLY, panel, 0)
    late = held.at[:, pl.ds(EARLY, LATE)]
    pltpu.make_async_copy(late, late, late_sem).wait()
    lax.fori_loop(EARLY, PANELS, panel, 0)


def solve(place, rows, arrays):
    return pl.pallas_call(
        kernel,
        out_shape=jax.ShapeDtypeStruct((PANELS, ROWS, PANEL), jnp.float32),
        in_specs=[pl.BlockSpec(memory_space=pltpu.SMEM), pl.BlockSpec(memory_space=pltpu.VMEM)]
        + [pl.BlockSpec(memory_space=pltpu.HBM)] * len(arrays),
        out_specs=pl.BlockSpec(memory_space=pltpu.VMEM),
        scratch_shapes=[
            pltpu.VMEM((32, SLOTS, 8, 32, LANES), jnp.float32),
            pltpu.VMEM((ROWS, PANEL), jnp.float32),
            pltpu.VMEM((PANELS, 2 * ROWS, PANEL), jnp.bfloat16),
            pltpu.SemaphoreType.DMA,
            pltpu.SemaphoreType.DMA,
        ],
        compiler_params=pltpu.CompilerParams(vmem_limit_bytes=48 * 2**20),
        cost_estimate=pl.CostEstimate(flops=16 * 10**9, bytes_accessed=40 * 10**6, transcendentals=0),
    )(place, rows, *arrays)


def local(integrals, factor, diag_inverse):
    pair, aux = lax.axis_index("pair"), lax.axis_index("aux")
    x, z, core = pair // 8, (pair // 2) % 4 * 2 + aux // NY, pair % 2
    place = jnp.stack([x, aux % NY, z, core]).astype(jnp.int32)

    piece = pieces(factor, diag_inverse, pair, aux)
    rows, (early, late) = gather(ring_of_eight(piece), integrals)
    arrays = early + [shift(v, core=1) for v in early] + late + [shift(v, core=1) for v in late]
    solved = solve(place, rows, arrays)
    result = lax.all_to_all(solved, "aux", 0, 0, tiled=True)
    return result.reshape(1, 8 * ROWS, PANEL)


def solution(mesh):
    in_specs = (P(None, "aux", "pair"), P("aux", "pair"), P("aux", None, None))
    out_specs = P("pair", None, "aux")
    return jax.shard_map(local, mesh=mesh, in_specs=in_specs, out_specs=out_specs, check_vma=False)
```

```python
import functools
import jax
import jax.numpy as jnp
from jax import lax
from jax.experimental import pallas as pl
from jax.experimental.pallas import tpu as pltpu
from jax.sharding import PartitionSpec as P

NX, NY, NZ = 4, 4, 8
ALL = ("pair", "aux")
EARLY, LATE = 4, 3
SLOTS = EARLY + LATE
PANELS, PANEL, LANES, ROWS = 8, 512, 128, 80
STEPS = (0, -1, 1, 2)


def device_id(x, y, z, core):
    return ((x * NZ // 2 + z // 2) * 2 + core) * 8 + (z % 2) * NY + y


def shift(value, dx=0, dy=0, dz=0, core=0):
    pairs = [
        (device_id(x, y, z, c), device_id((x + dx) % NX, (y + dy) % NY, (z + dz) % NZ, (c + core) % 2))
        for x in range(NX)
        for y in range(NY)
        for z in range(NZ)
        for c in range(2)
    ]
    return lax.ppermute(value, ALL, pairs)


def along(axis):
    return lambda value, d: shift(value, **{axis: d})


def ring_of_eight(piece):
    up, down = [piece], [piece]
    for _ in range(3):
        up.append(shift(up[-1], dz=1))
        down.append(shift(down[-1], dz=-1))
    far = jnp.concatenate([shift(up[3][:EARLY], dz=1), shift(down[3][EARLY:], dz=-1)])
    return jnp.stack(up + [far] + down[:0:-1])


def swap(values):
    return [shift(value, core=1) for value in values]


def start(integrals, factor, diag_inverse, pair):
    chunks = factor.reshape(2, 8, 32, LANES).transpose(1, 0, 2, 3)
    chunks = lax.all_to_all(chunks, "aux", 0, 0, tiled=True)
    half = lax.dynamic_slice(diag_inverse[0], (256 * (pair % 2), 0), (256, PANEL))
    chunks, half, integrals = lax.optimization_barrier((chunks, half, integrals))
    other = lax.ppermute(chunks[:, 1], "pair", [(p, 4 * (7 - p // 4) + p % 4) for p in range(32)])
    neighbour = lax.ppermute(half, "aux", [(a, (a + 4) % 8) for a in range(8)])
    rows = lax.all_to_all(integrals, "pair", 0, 0, tiled=True)
    other, neighbour = lax.optimization_barrier((other, neighbour))
    own = jnp.stack([half, neighbour])
    up, down = shift(own, dy=1), shift(own, dy=-1)
    column = ring_of_eight(share(chunks[:, 0], other, pair // 4))
    column, rows, up, down = lax.optimization_barrier((column, rows, up, down))
    far = jnp.stack([shift(up[0], dy=1), shift(down[1], dy=-1)])
    return rows, column, (own, up, down, far)


def share(own, other, column):
    is_low = column < 4
    low = jnp.where(is_low, own, other)
    high = jnp.where(is_low, other, own)
    both = jnp.concatenate([low, high])
    least = jnp.minimum(column, 7 - column)
    held = []
    for slot in range(SLOTS):
        paired = (slot + 9) // 2 if slot % 2 else 8 + (slot + 8) // 2
        index = jnp.where(slot < 7 - 2 * least, slot + least + 1, paired)
        held.append(lax.dynamic_index_in_dim(both, index, 0, keepdims=False))
    return jnp.stack(held)


def swap(values):
    return [shift(value, core=1) for value in values]


def gather(column, diagonals):
    blocks = [column[:, :EARLY], column[:, EARLY:]]
    first = [along("dx"), along("dy")]
    second = [along("dy"), along("dx")]
    near = [(one(block, 1), one(block, -1)) for one, block in zip(first, blocks)]
    near = lax.optimization_barrier(near)
    far = [(one(up[:4], 1), one(down[4:], -1)) for one, (up, down) in zip(first, near)]
    whole = [jnp.concatenate([block, up, down, *ends]) for block, (up, down), ends in zip(blocks, near, far)]
    whole, diagonals = lax.optimization_barrier((whole, diagonals))
    near = [(two(block, 1), two(block, -1)) for two, block in zip(second, whole)]
    diagonals = jnp.stack(diagonals)
    swapped = swap([*whole, diagonals])
    near, swapped = lax.optimization_barrier((near, swapped))
    far = [(two(up[:16], 1), two(down[16:], -1)) for two, (up, down) in zip(second, near)]
    swapped_near = [swap(values) for values in near]
    far, swapped_near = lax.optimization_barrier((far, swapped_near))
    gathered = []
    for color in range(2):
        gathered += [whole[color], *near[color], *far[color]]
        gathered += [swapped[color], *swapped_near[color], *swap(far[color])]
    return (diagonals, swapped[2]), gathered


LAYOUT = ((0, 0, 32), (-1, 0, 32), (1, 0, 32), (-2, 0, 16), (2, 16, 16))


def kernel(*refs):
    place_ref, x_ref, diagonals, swapped_diagonals = refs[:4]
    arrays = refs[4:24]
    out_ref, held, inverses, remain, parts, inverse_sem, early_sem, late_sem = refs[24:]
    x, y, z, core = (place_ref[i] for i in range(4))

    for ref, from_core in ((diagonals, core), (swapped_diagonals, 1 - core)):
        for at in range(4):
            for other in range(2):
                sy = lax.rem(y + STEPS[at] + NY, NY)
                group = lax.rem(z + other, 2) * NY + sy
                rows = pl.ds(pl.multiple_of(256 * from_core, 256), 256)
                pltpu.make_async_copy(ref.at[at, other], inverses.at[group, rows], inverse_sem).start()

    def fetch(ref, second, start, count, x_first, from_core, first_slot, sem):
        for block in range(4):
            low, high = max(start, 8 * block), min(start + count, 8 * block + 8)
            if low >= high:
                continue
            dx, dy = (STEPS[block], second) if x_first else (second, STEPS[block])
            sx, sy = lax.rem(x + dx + NX, NX), lax.rem(y + dy + NY, NY)

            @pl.loop(low, high)
            def _(number):
                sz = lax.rem(z - (number - 8 * block) + NZ, NZ)
                holder = sx * 8 + lax.div(sz, 2) * 2 + from_core
                group = lax.rem(sz, 2) * NY + sy
                slots = pl.ds(first_slot, ref.shape[1])
                pltpu.make_async_copy(ref.at[number - start], held.at[holder, slots, group], sem).start()

    for color, (first_slot, sem) in enumerate(((0, early_sem), (EARLY, late_sem))):
        for which, from_core in enumerate((core, 1 - core)):
            for number, (second, start, count) in enumerate(LAYOUT):
                ref = arrays[10 * color + 5 * which + number]
                fetch(ref, second, start, count, color == 0, from_core, first_slot, sem)

    def product(left, load):
        halves = []
        for half in range(2):
            total = None
            for side in range(2):
                weight = load(half, side)
                high = weight.astype(jnp.bfloat16)
                low = (weight - high.astype(jnp.float32)).astype(jnp.bfloat16)
                part = left[:, 256 * side : 256 * (side + 1)]
                dims = (((1,), (1,)), ((), ()))
                twice = lax.dot_general(part, high, dims, preferred_element_type=jnp.float32)
                once = lax.dot_general(part[:ROWS], low, dims, preferred_element_type=jnp.float32)
                piece = twice[:ROWS] + (twice[ROWS:] + once)
                total = piece if total is None else total + piece
            halves.append(total)
        return jnp.concatenate(halves, axis=1)

    def split(value):
        high = value.astype(jnp.bfloat16)
        low = (value - high.astype(jnp.float32)).astype(jnp.bfloat16)
        return jnp.concatenate([high, low], axis=0)

    def panel(j, carry):
        remain[...] = jnp.concatenate([x_ref[4 * j + s] for s in range(4)], axis=1)

        def update(k, carry):
            low_slot = jnp.where(j < 8 - k, j - k - 1, 2 * j - 9)
            slot = jnp.where(k < 4, low_slot, 2 * j - 8)

            def load(half, side):
                first = (4 * (7 - k) if half else 4 * k) + 2 * side
                return jnp.concatenate([held[first + s, slot].reshape(256, LANES) for s in range(2)], axis=1)

            remain[...] -= product(parts[k], load)
            return carry

        lax.fori_loop(0, j, update, 0)

        def load(half, side):
            return inverses[j, 256 * half : 256 * (half + 1), 256 * side : 256 * (side + 1)]

        solved = product(split(remain[...]), load)
        out_ref[j] = solved
        parts[j] = split(solved)
        return carry

    pltpu.make_async_copy(inverses, inverses, inverse_sem).wait()
    early = held.at[:, pl.ds(0, EARLY)]
    pltpu.make_async_copy(early, early, early_sem).wait()
    lax.fori_loop(0, EARLY + 1, panel, 0)
    late = held.at[:, pl.ds(EARLY, LATE)]
    pltpu.make_async_copy(late, late, late_sem).wait()
    lax.fori_loop(EARLY + 1, PANELS, panel, 0)


def solve(place, rows, diagonals, arrays):
    return pl.pallas_call(
        kernel,
        out_shape=jax.ShapeDtypeStruct((PANELS, ROWS, PANEL), jnp.float32),
        in_specs=[pl.BlockSpec(memory_space=pltpu.SMEM), pl.BlockSpec(memory_space=pltpu.VMEM)]
        + [pl.BlockSpec(memory_space=pltpu.HBM)] * (len(diagonals) + len(arrays)),
        out_specs=pl.BlockSpec(memory_space=pltpu.VMEM),
        scratch_shapes=[
            pltpu.VMEM((32, SLOTS, 8, 32, LANES), jnp.float32),
            pltpu.VMEM((PANELS, PANEL, PANEL), jnp.float32),
            pltpu.VMEM((ROWS, PANEL), jnp.float32),
            pltpu.VMEM((PANELS, 2 * ROWS, PANEL), jnp.bfloat16),
            pltpu.SemaphoreType.DMA,
            pltpu.SemaphoreType.DMA,
            pltpu.SemaphoreType.DMA,
        ],
        compiler_params=pltpu.CompilerParams(vmem_limit_bytes=48 * 2**20),
        cost_estimate=pl.CostEstimate(flops=16 * 10**9, bytes_accessed=40 * 10**6, transcendentals=0),
    )(place, rows, *diagonals, *arrays)


def local(integrals, factor, diag_inverse):
    pair, aux = lax.axis_index("pair"), lax.axis_index("aux")
    x, z, core = pair // 8, (pair // 2) % 4 * 2 + aux // NY, pair % 2
    place = jnp.stack([x, aux % NY, z, core]).astype(jnp.int32)

    rows, column, diagonals = start(integrals, factor, diag_inverse, pair)
    solved = solve(place, rows, *gather(column, diagonals))
    result = lax.all_to_all(solved, "aux", 0, 0, tiled=True)
    return result.reshape(1, 8 * ROWS, PANEL)


def solution(mesh):
    in_specs = (P(None, "aux", "pair"), P("aux", "pair"), P("aux", None, None))
    out_specs = P("pair", None, "aux")
    return jax.shard_map(local, mesh=mesh, in_specs=in_specs, out_specs=out_specs, check_vma=False)
```

```python
import functools
import jax
import jax.numpy as jnp
from jax import lax
from jax.experimental import pallas as pl
from jax.experimental.pallas import tpu as pltpu
from jax.sharding import PartitionSpec as P

NX, NY, NZ = 4, 4, 8
ALL = ("pair", "aux")
EARLY, LATE = 4, 3
SLOTS = EARLY + LATE
PANELS, PANEL, LANES, ROWS = 8, 512, 128, 80
STEPS = (0, -1, 1, 2)


def device_id(x, y, z, core):
    return ((x * NZ // 2 + z // 2) * 2 + core) * 8 + (z % 2) * NY + y


def shift(value, dx=0, dy=0, dz=0, core=0):
    pairs = [
        (device_id(x, y, z, c), device_id((x + dx) % NX, (y + dy) % NY, (z + dz) % NZ, (c + core) % 2))
        for x in range(NX)
        for y in range(NY)
        for z in range(NZ)
        for c in range(2)
    ]
    return lax.ppermute(value, ALL, pairs)


def along(axis):
    return lambda value, d: shift(value, **{axis: d})


def ring_of_eight(piece):
    up, down = [piece], [piece]
    for _ in range(3):
        up.append(shift(up[-1], dz=1))
        down.append(shift(down[-1], dz=-1))
    far = jnp.concatenate([shift(up[3][:EARLY], dz=1), shift(down[3][EARLY:], dz=-1)])
    return jnp.stack(up + [far] + down[:0:-1])


def swap(values):
    return [shift(value, core=1) for value in values]


def start(factor, diag_inverse, pair):
    chunks = factor.reshape(2, 8, 32, LANES).transpose(1, 0, 2, 3)
    chunks = lax.all_to_all(chunks, "aux", 0, 0, tiled=True)
    half = lax.dynamic_slice(diag_inverse[0], (256 * (pair % 2), 0), (256, PANEL))
    chunks, half = lax.optimization_barrier((chunks, half))
    other = lax.ppermute(chunks[:, 1], "pair", [(p, 4 * (7 - p // 4) + p % 4) for p in range(32)])
    neighbour = lax.ppermute(half, "aux", [(a, (a + 4) % 8) for a in range(8)])
    other, neighbour = lax.optimization_barrier((other, neighbour))
    own = jnp.stack([half, neighbour])
    up, down = shift(own, dy=1), shift(own, dy=-1)
    column = ring_of_eight(share(chunks[:, 0], other, pair // 4))
    column, up, down = lax.optimization_barrier((column, up, down))
    return column, [own, up, down]


def share(own, other, column):
    is_low = column < 4
    low = jnp.where(is_low, own, other)
    high = jnp.where(is_low, other, own)
    both = jnp.concatenate([low, high])
    least = jnp.minimum(column, 7 - column)
    held = []
    for slot in range(SLOTS):
        paired = (slot + 9) // 2 if slot % 2 else 8 + (slot + 8) // 2
        index = jnp.where(slot < 7 - 2 * least, slot + least + 1, paired)
        held.append(lax.dynamic_index_in_dim(both, index, 0, keepdims=False))
    return jnp.stack(held)


def swap(values):
    return [shift(value, core=1) for value in values]


def gather(column, diagonals, integrals):
    blocks = [column[:, :EARLY], column[:, EARLY:]]
    first = [along("dx"), along("dy")]
    second = [along("dy"), along("dx")]
    near = [(one(block, 1), one(block, -1)) for one, block in zip(first, blocks)]
    near, diagonals = lax.optimization_barrier((near, diagonals))
    far = [(one(up[:4], 1), one(down[4:], -1)) for one, (up, down) in zip(first, near)]
    ends = jnp.stack([shift(diagonals[1][0], dy=1), shift(diagonals[2][1], dy=-1)])
    whole = [jnp.concatenate([block, up, down, *ends]) for block, (up, down), ends in zip(blocks, near, far)]
    whole, ends, integrals = lax.optimization_barrier((whole, ends, integrals))
    near = [(two(block, 1), two(block, -1)) for two, block in zip(second, whole)]
    rows = lax.all_to_all(integrals, "pair", 0, 0, tiled=True)
    diagonals = jnp.stack([*diagonals, ends])
    swapped = swap([*whole, diagonals])
    near, swapped, rows = lax.optimization_barrier((near, swapped, rows))
    far = [(two(up[:16], 1), two(down[16:], -1)) for two, (up, down) in zip(second, near)]
    swapped_near = [swap(values) for values in near]
    far, swapped_near = lax.optimization_barrier((far, swapped_near))
    gathered = []
    for color in range(2):
        gathered += [whole[color], *near[color], *far[color]]
        gathered += [swapped[color], *swapped_near[color], *swap(far[color])]
    return rows, (diagonals, swapped[2]), gathered


LAYOUT = ((0, 0, 32), (-1, 0, 32), (1, 0, 32), (-2, 0, 16), (2, 16, 16))


def kernel(*refs):
    place_ref, x_ref, diagonals, swapped_diagonals = refs[:4]
    arrays = refs[4:24]
    out_ref, held, inverses, remain, parts, inverse_sem, early_sem, late_sem = refs[24:]
    x, y, z, core = (place_ref[i] for i in range(4))

    for ref, from_core in ((diagonals, core), (swapped_diagonals, 1 - core)):
        for at in range(4):
            for other in range(2):
                sy = lax.rem(y + STEPS[at] + NY, NY)
                group = lax.rem(z + other, 2) * NY + sy
                rows = pl.ds(pl.multiple_of(256 * from_core, 256), 256)
                pltpu.make_async_copy(ref.at[at, other], inverses.at[group, rows], inverse_sem).start()

    def fetch(ref, second, start, count, x_first, from_core, first_slot, sem):
        @pl.loop(start, start + count)
        def _(number):
            block = lax.div(number, NZ)
            step = jnp.where(block == 3, 2, jnp.where(block == 1, -1, jnp.minimum(block, 1)))
            dx, dy = (step, second) if x_first else (second, step)
            sx, sy = lax.rem(x + dx + NX, NX), lax.rem(y + dy + NY, NY)
            sz = lax.rem(z - lax.rem(number, NZ) + NZ, NZ)
            holder = sx * 8 + lax.div(sz, 2) * 2 + from_core
            group = lax.rem(sz, 2) * NY + sy
            slots = pl.ds(first_slot, ref.shape[1])
            pltpu.make_async_copy(ref.at[number - start], held.at[holder, slots, group], sem).start()

    for color, (first_slot, sem) in enumerate(((0, early_sem), (EARLY, late_sem))):
        for which, from_core in enumerate((core, 1 - core)):
            for number, (second, start, count) in enumerate(LAYOUT):
                ref = arrays[10 * color + 5 * which + number]
                fetch(ref, second, start, count, color == 0, from_core, first_slot, sem)

    def product(left, load):
        halves = []
        for half in range(2):
            total = None
            for side in range(2):
                weight = load(half, side)
                high = weight.astype(jnp.bfloat16)
                low = (weight - high.astype(jnp.float32)).astype(jnp.bfloat16)
                part = left[:, 256 * side : 256 * (side + 1)]
                dims = (((1,), (1,)), ((), ()))
                twice = lax.dot_general(part, high, dims, preferred_element_type=jnp.float32)
                once = lax.dot_general(part[:ROWS], low, dims, preferred_element_type=jnp.float32)
                piece = twice[:ROWS] + (twice[ROWS:] + once)
                total = piece if total is None else total + piece
            halves.append(total)
        return jnp.concatenate(halves, axis=1)

    def split(value):
        high = value.astype(jnp.bfloat16)
        low = (value - high.astype(jnp.float32)).astype(jnp.bfloat16)
        return jnp.concatenate([high, low], axis=0)

    def panel(j, carry):
        @pl.when(j == EARLY + 1)
        def _():
            late = held.at[:, pl.ds(EARLY, LATE)]
            pltpu.make_async_copy(late, late, late_sem).wait()

        remain[...] = jnp.concatenate([x_ref[4 * j + s] for s in range(4)], axis=1)

        def update(k, carry):
            low_slot = jnp.where(j < 8 - k, j - k - 1, 2 * j - 9)
            slot = jnp.where(k < 4, low_slot, 2 * j - 8)

            def load(half, side):
                first = (4 * (7 - k) if half else 4 * k) + 2 * side
                return jnp.concatenate([held[first + s, slot].reshape(256, LANES) for s in range(2)], axis=1)

            remain[...] -= product(parts[k], load)
            return carry

        lax.fori_loop(0, j, update, 0)

        def load(half, side):
            return inverses[j, 256 * half : 256 * (half + 1), 256 * side : 256 * (side + 1)]

        solved = product(split(remain[...]), load)
        out_ref[j] = solved
        parts[j] = split(solved)
        return carry

    pltpu.make_async_copy(inverses, inverses, inverse_sem).wait()
    early = held.at[:, pl.ds(0, EARLY)]
    pltpu.make_async_copy(early, early, early_sem).wait()
    lax.fori_loop(0, PANELS, panel, 0)


def solve(place, rows, diagonals, arrays):
    return pl.pallas_call(
        kernel,
        out_shape=jax.ShapeDtypeStruct((PANELS, ROWS, PANEL), jnp.float32),
        in_specs=[pl.BlockSpec(memory_space=pltpu.SMEM), pl.BlockSpec(memory_space=pltpu.VMEM)]
        + [pl.BlockSpec(memory_space=pl.ANY)] * (len(diagonals) + len(arrays)),
        out_specs=pl.BlockSpec(memory_space=pltpu.VMEM),
        scratch_shapes=[
            pltpu.VMEM((32, SLOTS, 8, 32, LANES), jnp.float32),
            pltpu.VMEM((PANELS, PANEL, PANEL), jnp.float32),
            pltpu.VMEM((ROWS, PANEL), jnp.float32),
            pltpu.VMEM((PANELS, 2 * ROWS, PANEL), jnp.bfloat16),
            pltpu.SemaphoreType.DMA,
            pltpu.SemaphoreType.DMA,
            pltpu.SemaphoreType.DMA,
        ],
        compiler_params=pltpu.CompilerParams(vmem_limit_bytes=48 * 2**20),
        cost_estimate=pl.CostEstimate(flops=16 * 10**9, bytes_accessed=40 * 10**6, transcendentals=0),
    )(place, rows, *diagonals, *arrays)


def local(integrals, factor, diag_inverse):
    pair, aux = lax.axis_index("pair"), lax.axis_index("aux")
    x, z, core = pair // 8, (pair // 2) % 4 * 2 + aux // NY, pair % 2
    place = jnp.stack([x, aux % NY, z, core]).astype(jnp.int32)

    column, diagonals = start(factor, diag_inverse, pair)
    rows, diagonals, gathered = gather(column, diagonals, integrals)
    solved = solve(place, rows, diagonals, gathered)
    result = lax.all_to_all(solved, "aux", 0, 0, tiled=True)
    return result.reshape(1, 8 * ROWS, PANEL)


def solution(mesh):
    in_specs = (P(None, "aux", "pair"), P("aux", "pair"), P("aux", None, None))
    out_specs = P("pair", None, "aux")
    return jax.shard_map(local, mesh=mesh, in_specs=in_specs, out_specs=out_specs, check_vma=False)
```

```python
import jax
import jax.numpy as jnp
from jax import lax
from jax.experimental import pallas as pl
from jax.experimental.pallas import tpu as pltpu
from jax.sharding import PartitionSpec as P


NX, NY, NZ = 4, 4, 8
ALL = ("pair", "aux")
EARLY, LATE = 4, 3
SLOTS = EARLY + LATE
PANELS, PANEL, LANES, ROWS = 8, 512, 128, 80


def device_id(x, y, z, core):
    return ((x * NZ // 2 + z // 2) * 2 + core) * 8 + (z % 2) * NY + y


def shift(value, dx=0, dy=0, dz=0, core=0):
    pairs = [
        (device_id(x, y, z, c), device_id((x + dx) % NX, (y + dy) % NY, (z + dz) % NZ, (c + core) % 2))
        for x in range(NX)
        for y in range(NY)
        for z in range(NZ)
        for c in range(2)
    ]
    return lax.ppermute(value, ALL, pairs)


def along(axis):
    return lambda value, d: shift(value, **{axis: d})


def ring_of_eight(piece):
    near = [shift(piece, dz=d) for d in (1, -1, 2, -2)]
    one, minus_one, two, minus_two = lax.optimization_barrier(near)
    three, minus_three = shift(two, dz=1), shift(minus_two, dz=-1)
    four = jnp.concatenate([shift(two[:EARLY], dz=2), shift(minus_two[EARLY:], dz=-2)])
    return jnp.stack([piece, one, two, three, four, minus_three, minus_two, minus_one])


def spread(factor, pair):
    halves = factor.reshape(2, 8, 32, LANES)
    halves = jnp.where(pair < 16, halves, halves[::-1]).reshape(16, 32, LANES)
    groups = [[8 * p + a for p in (low, 31 - low) for a in range(8)] for low in range(16)]
    return lax.all_to_all(halves, ALL, 0, 0, axis_index_groups=groups, tiled=True)


def share(both, column):
    least = jnp.minimum(column, 7 - column)
    held = []
    for slot in range(SLOTS):
        paired = (slot + 9) // 2 if slot % 2 else 8 + (slot + 8) // 2
        index = jnp.where(slot < 7 - 2 * least, slot + least + 1, paired)
        held.append(lax.dynamic_index_in_dim(both, index, 0, keepdims=False))
    return jnp.stack(held)


def start(factor, diag_inverse, pair):
    half = lax.dynamic_slice(diag_inverse[0], (256 * (pair % 2), 0), (256, PANEL))
    neighbour = lax.ppermute(half, "aux", [(a, (a + 4) % 8) for a in range(8)])
    both = spread(factor, pair)
    both, neighbour = lax.optimization_barrier((both, neighbour))
    own = jnp.stack([half, neighbour])
    up, down = shift(own, dy=1), shift(own, dy=-1)
    column = ring_of_eight(share(both, pair // 4))
    column, up, down = lax.optimization_barrier((column, up, down))
    return column, [own, up, down]


def swap(values):
    return [shift(value, core=1) for value in values]


def gather(column, diagonals, integrals):
    blocks = [column[:, :EARLY], column[:, EARLY:]]
    first = [along("dx"), along("dy")]
    second = [along("dy"), along("dx")]
    near = [(one(block, 1), one(block, -1)) for one, block in zip(first, blocks)]
    near, diagonals = lax.optimization_barrier((near, diagonals))
    far = [(one(up[:4], 1), one(down[4:], -1)) for one, (up, down) in zip(first, near)]
    ends = jnp.stack([shift(diagonals[1][0], dy=1), shift(diagonals[2][1], dy=-1)])
    whole = [jnp.concatenate([block, up, down, *ends]) for block, (up, down), ends in zip(blocks, near, far)]
    whole, ends, integrals = lax.optimization_barrier((whole, ends, integrals))
    near = [(two(block, 1), two(block, -1)) for two, block in zip(second, whole)]
    swapped = swap(whole)
    swapped, diagonals, ends = lax.optimization_barrier((swapped, diagonals, ends))
    rows = lax.all_to_all(integrals, "pair", 0, 0, tiled=True)
    diagonals = jnp.stack([*diagonals, ends])
    swapped += swap([diagonals])
    near, swapped, rows = lax.optimization_barrier((near, swapped, rows))
    far = [(two(up[:16], 1), two(down[16:], -1)) for two, (up, down) in zip(second, near)]
    swapped_near = [swap(values) for values in near]
    far, swapped_near = lax.optimization_barrier((far, swapped_near))
    gathered = []
    for color in range(2):
        gathered += [whole[color], *near[color], *far[color]]
        gathered += [swapped[color], *swapped_near[color], *swap(far[color])]
    return rows, (diagonals, swapped[2]), gathered


LAYOUT = ((0, 0, 4), (1, 0, 4), (2, 0, 4), (3, 0, 2), (3, 2, 2))


def position(delta):
    delta = lax.rem(delta + 4, 4)
    return jnp.where(delta == 3, 1, jnp.where(delta == 0, 0, delta + 1))


def kernel(*refs):
    place_ref, x_ref = refs[:2]
    diagonals, arrays = refs[2:4], refs[4:24]
    out_ref, held, inverses, remain, parts, inverse_sem, early_sem, late_sem = refs[24:]
    x, y, z, core = (place_ref[i] for i in range(4))

    for other in range(2):
        pltpu.make_async_copy(diagonals[other], inverses.at[other], inverse_sem).start()
    for other in range(2):
        for number, (second, block, count) in enumerate(LAYOUT):
            ref = arrays[5 * other + number]
            to = held.at[other, second, pl.ds(block, count), :, pl.ds(0, EARLY)]
            pltpu.make_async_copy(ref, to, early_sem).start()
    for other in range(2):
        for number, (second, block, count) in enumerate(LAYOUT):
            ref = arrays[10 + 5 * other + number]
            to = held.at[other, pl.ds(block, count), second, :, pl.ds(EARLY, LATE)]
            pltpu.make_async_copy(ref, to, late_sem).start()
    y_positions = [position(sy - y) for sy in range(NY)]

    def slab(p, slot):
        x_position = position(lax.div(p, 8) - x)
        other = lax.rem(p + core, 2)
        sz = 2 * lax.rem(lax.div(p, 2), 4)
        rows = []
        for z_lo in range(2):
            d = lax.rem(z - sz - z_lo + NZ, NZ)
            rows += [held[other, y_positions[sy], x_position, d, slot] for sy in range(NY)]
        return jnp.concatenate(rows)

    def product(left, load):
        halves = []
        for half in range(2):
            total = None
            for side in range(2):
                weight = load(half, side)
                high = weight.astype(jnp.bfloat16)
                low = (weight - high.astype(jnp.float32)).astype(jnp.bfloat16)
                part = left[:, 256 * side : 256 * (side + 1)]
                dims = (((1,), (1,)), ((), ()))
                twice = lax.dot_general(part, high, dims, preferred_element_type=jnp.float32)
                once = lax.dot_general(part[:ROWS], low, dims, preferred_element_type=jnp.float32)
                piece = twice[:ROWS] + (twice[ROWS:] + once)
                total = piece if total is None else total + piece
            halves.append(total)
        return jnp.concatenate(halves, axis=1)

    def split(value):
        high = value.astype(jnp.bfloat16)
        low = (value - high.astype(jnp.float32)).astype(jnp.bfloat16)
        return jnp.concatenate([high, low], axis=0)

    def panel(j, carry):
        @pl.when(j == EARLY + 1)
        def _():
            late = held.at[:, :, :, :, pl.ds(EARLY, LATE)]
            pltpu.make_async_copy(late, late, late_sem).wait()

        remain[...] = jnp.concatenate([x_ref[4 * j + s] for s in range(4)], axis=1)

        def update(k, carry):
            low_slot = jnp.where(j < 8 - k, j - k - 1, 2 * j - 9)
            slot = jnp.where(k < 4, low_slot, 2 * j - 8)

            def load(half, side):
                columns = [4 * k + 2 * side + s for s in range(2)]
                return jnp.concatenate([slab(31 - p if half else p, slot) for p in columns], axis=1)

            remain[...] -= product(parts[k], load)
            return carry

        lax.fori_loop(0, j, update, 0)

        def load(half, side):
            other, z_lo = lax.rem(core + half, 2), lax.rem(z + lax.div(j, 4), 2)
            at = position(lax.rem(j, 4) - y)
            return inverses[other, at, z_lo, :, 256 * side : 256 * (side + 1)]

        solved = product(split(remain[...]), load)
        out_ref[j] = solved
        parts[j] = split(solved)
        return carry

    pltpu.make_async_copy(inverses, inverses, inverse_sem).wait()
    early = held.at[:, :, :, :, pl.ds(0, EARLY)]
    pltpu.make_async_copy(early, early, early_sem).wait()
    lax.fori_loop(0, PANELS, panel, 0)


def solve(place, rows, diagonals, arrays):
    arrays = [v.reshape(-1, NZ, *v.shape[1:]) for v in arrays]
    return pl.pallas_call(
        kernel,
        out_shape=jax.ShapeDtypeStruct((PANELS, ROWS, PANEL), jnp.float32),
        in_specs=[pl.BlockSpec(memory_space=pltpu.SMEM), pl.BlockSpec(memory_space=pltpu.VMEM)]
        + [pl.BlockSpec(memory_space=pl.ANY)] * (len(diagonals) + len(arrays)),
        out_specs=pl.BlockSpec(memory_space=pltpu.VMEM),
        scratch_shapes=[
            pltpu.VMEM((2, 4, 4, NZ, SLOTS, 32, LANES), jnp.float32),
            pltpu.VMEM((2, 4, 2, 256, PANEL), jnp.float32),
            pltpu.VMEM((ROWS, PANEL), jnp.float32),
            pltpu.VMEM((PANELS, 2 * ROWS, PANEL), jnp.bfloat16),
            pltpu.SemaphoreType.DMA,
            pltpu.SemaphoreType.DMA,
            pltpu.SemaphoreType.DMA,
        ],
        compiler_params=pltpu.CompilerParams(vmem_limit_bytes=48 * 2**20),
        cost_estimate=pl.CostEstimate(flops=16 * 10**9, bytes_accessed=40 * 10**6, transcendentals=0),
    )(place, rows, *diagonals, *arrays)


def local(integrals, factor, diag_inverse):
    pair, aux = lax.axis_index("pair"), lax.axis_index("aux")
    x, z, core = pair // 8, (pair // 2) % 4 * 2 + aux // NY, pair % 2
    place = jnp.stack([x, aux % NY, z, core]).astype(jnp.int32)

    column, diagonals = start(factor, diag_inverse, pair)
    rows, diagonals, gathered = gather(column, diagonals, integrals)
    solved = solve(place, rows, diagonals, gathered)
    result = lax.all_to_all(solved, "aux", 0, 0, tiled=True)
    return result.reshape(1, 8 * ROWS, PANEL)


def solution(mesh):
    in_specs = (P(None, "aux", "pair"), P("aux", "pair"), P("aux", None, None))
    out_specs = P("pair", None, "aux")
    return jax.shard_map(local, mesh=mesh, in_specs=in_specs, out_specs=out_specs, check_vma=False)
```

```python
import jax
import jax.numpy as jnp
from jax import lax
from jax.experimental import pallas as pl
from jax.experimental.pallas import tpu as pltpu
from jax.sharding import PartitionSpec as P


NX, NY, NZ = 4, 4, 8
ALL = ("pair", "aux")
EARLY, LATE = 4, 3
SLOTS = EARLY + LATE
PANELS, PANEL, LANES, ROWS = 8, 512, 128, 80


def device_id(x, y, z, core):
    return ((x * NZ // 2 + z // 2) * 2 + core) * 8 + (z % 2) * NY + y


def shift(value, dx=0, dy=0, dz=0, core=0):
    pairs = [
        (device_id(x, y, z, c), device_id((x + dx) % NX, (y + dy) % NY, (z + dz) % NZ, (c + core) % 2))
        for x in range(NX)
        for y in range(NY)
        for z in range(NZ)
        for c in range(2)
    ]
    return lax.ppermute(value, ALL, pairs)


def along(axis):
    return lambda value, d: shift(value, **{axis: d})


def ring_of_eight(piece):
    near = [shift(piece, dz=d) for d in (1, -1, 2, -2)]
    one, minus_one, two, minus_two = lax.optimization_barrier(near)
    three, minus_three = shift(two, dz=1), shift(minus_two, dz=-1)
    four = shift(two, dz=2)
    return jnp.stack([piece, one, two, three, four, minus_three, minus_two, minus_one])


def spread(factor, pair):
    halves = factor.reshape(2, 8, 32, LANES)
    halves = jnp.where(pair < 16, halves, halves[::-1]).reshape(16, 32, LANES)
    groups = [[8 * p + a for p in (low, 31 - low) for a in range(8)] for low in range(16)]
    return lax.all_to_all(halves, ALL, 0, 0, axis_index_groups=groups, tiled=True)


def share(both, column):
    least = jnp.minimum(column, 7 - column)
    held = []
    for slot in range(SLOTS):
        paired = (slot + 9) // 2 if slot % 2 else 8 + (slot + 8) // 2
        index = jnp.where(slot < 7 - 2 * least, slot + least + 1, paired)
        held.append(lax.dynamic_index_in_dim(both, index, 0, keepdims=False))
    return jnp.stack(held)


def swap(values):
    return [shift(value, core=1) for value in values]


def gather(column, half, integrals):
    blocks = [column[:, :EARLY], column[:, EARLY:]]
    first = [along("dy"), along("dx")]
    second = [along("dx"), along("dy")]
    near = [(one(block, 1), one(block, -1)) for one, block in zip(first, blocks)]
    neighbour = lax.ppermute(half, "aux", [(a, (a + 4) % 8) for a in range(8)])
    near = lax.optimization_barrier(near)
    far = [(one(up[:4], 1), one(down[4:], -1)) for one, (up, down) in zip(first, near)]
    whole = [jnp.concatenate([block, up, down, *ends]) for block, (up, down), ends in zip(blocks, near, far)]
    inverses = jnp.stack([half, neighbour])
    whole, inverses, integrals = lax.optimization_barrier((whole, inverses, integrals))
    near = [(two(block, 1), two(block, -1)) for two, block in zip(second, whole)]
    sides = shift(inverses, dy=1), shift(inverses, dy=-1)
    swapped = swap([*whole, inverses])
    rows = lax.all_to_all(integrals, "pair", 0, 0, tiled=True)
    near, swapped, rows, sides = lax.optimization_barrier((near, swapped, rows, sides))
    far = [(two(up[:16], 1), two(down[16:], -1)) for two, (up, down) in zip(second, near)]
    ends = shift(sides[0][0], dy=1), shift(sides[1][1], dy=-1)
    sides = jnp.stack(sides)
    swapped_near = [swap(values) for values in [*near, [sides]]]
    far, swapped_near, ends = lax.optimization_barrier((far, swapped_near, ends))
    ends = jnp.stack(ends)
    gathered = []
    for color in range(2):
        gathered += [whole[color], *near[color], *far[color]]
        gathered += [swapped[color], *swapped_near[color], *swap(far[color])]
    diagonals = [inverses, sides, ends, swapped[2], *swapped_near[2], *swap([ends])]
    return rows, diagonals, gathered


LAYOUT = ((0, 0, 4), (1, 0, 4), (2, 0, 4), (3, 0, 2), (3, 2, 2))


def position(delta):
    delta = lax.rem(delta + 4, 4)
    return jnp.where(delta == 3, 1, jnp.where(delta == 0, 0, delta + 1))


def kernel(*refs):
    place_ref, x_ref = refs[:2]
    diagonals, arrays = refs[2:8], refs[8:28]
    out_ref, held, inverses, remain, parts, inverse_sem, early_sem, late_sem = refs[28:]
    x, y, z, core = (place_ref[i] for i in range(4))

    for other in range(2):
        own, sides, ends = diagonals[3 * other : 3 * other + 3]
        pltpu.make_async_copy(own, inverses.at[other, 0], inverse_sem).start()
        pltpu.make_async_copy(sides, inverses.at[other, pl.ds(1, 2)], inverse_sem).start()
        pltpu.make_async_copy(ends, inverses.at[other, 3], inverse_sem).start()
    for other in range(2):
        for number, (second, block, count) in enumerate(LAYOUT):
            ref = arrays[5 * other + number]
            to = held.at[other, pl.ds(block, count), second, :, pl.ds(0, EARLY)]
            pltpu.make_async_copy(ref, to, early_sem).start()
    for other in range(2):
        for number, (second, block, count) in enumerate(LAYOUT):
            ref = arrays[10 + 5 * other + number]
            to = held.at[other, second, pl.ds(block, count), :, pl.ds(EARLY, LATE)]
            pltpu.make_async_copy(ref, to, late_sem).start()
    y_positions = [position(sy - y) for sy in range(NY)]

    def slab(p, slot):
        x_position = position(lax.div(p, 8) - x)
        other = lax.rem(p + core, 2)
        sz = 2 * lax.rem(lax.div(p, 2), 4)
        rows = []
        for z_lo in range(2):
            d = lax.rem(z - sz - z_lo + NZ, NZ)
            rows += [held[other, y_positions[sy], x_position, d, slot] for sy in range(NY)]
        return jnp.concatenate(rows)

    def product(left, load):
        halves = []
        for half in range(2):
            total = None
            for side in range(2):
                weight = load(half, side)
                high = weight.astype(jnp.bfloat16)
                low = (weight - high.astype(jnp.float32)).astype(jnp.bfloat16)
                part = left[:, 256 * side : 256 * (side + 1)]
                dims = (((1,), (1,)), ((), ()))
                twice = lax.dot_general(part, high, dims, preferred_element_type=jnp.float32)
                once = lax.dot_general(part[:ROWS], low, dims, preferred_element_type=jnp.float32)
                piece = twice[:ROWS] + (twice[ROWS:] + once)
                total = piece if total is None else total + piece
            halves.append(total)
        return jnp.concatenate(halves, axis=1)

    def split(value):
        high = value.astype(jnp.bfloat16)
        low = (value - high.astype(jnp.float32)).astype(jnp.bfloat16)
        return jnp.concatenate([high, low], axis=0)

    def panel(j, carry):
        @pl.when(j == EARLY + 1)
        def _():
            late = held.at[:, :, :, :, pl.ds(EARLY, LATE)]
            pltpu.make_async_copy(late, late, late_sem).wait()

        remain[...] = jnp.concatenate([x_ref[4 * j + s] for s in range(4)], axis=1)

        def update(k, carry):
            low_slot = jnp.where(j < 8 - k, j - k - 1, 2 * j - 9)
            slot = jnp.where(k < 4, low_slot, 2 * j - 8)

            def load(half, side):
                columns = [4 * k + 2 * side + s for s in range(2)]
                return jnp.concatenate([slab(31 - p if half else p, slot) for p in columns], axis=1)

            remain[...] -= product(parts[k], load)
            return carry

        lax.fori_loop(0, j, update, 0)

        def load(half, side):
            other, z_lo = lax.rem(core + half, 2), lax.rem(z + lax.div(j, 4), 2)
            at = position(lax.rem(j, 4) - y)
            return inverses[other, at, z_lo, :, 256 * side : 256 * (side + 1)]

        solved = product(split(remain[...]), load)
        out_ref[j] = solved
        parts[j] = split(solved)
        return carry

    pltpu.make_async_copy(inverses, inverses, inverse_sem).wait()
    early = held.at[:, :, :, :, pl.ds(0, EARLY)]
    pltpu.make_async_copy(early, early, early_sem).wait()
    lax.fori_loop(0, PANELS, panel, 0)


def solve(place, rows, diagonals, arrays):
    arrays = [v.reshape(-1, NZ, *v.shape[1:]) for v in arrays]
    return pl.pallas_call(
        kernel,
        out_shape=jax.ShapeDtypeStruct((PANELS, ROWS, PANEL), jnp.float32),
        in_specs=[pl.BlockSpec(memory_space=pltpu.SMEM), pl.BlockSpec(memory_space=pltpu.VMEM)]
        + [pl.BlockSpec(memory_space=pl.ANY)] * (len(diagonals) + len(arrays)),
        out_specs=pl.BlockSpec(memory_space=pltpu.VMEM),
        scratch_shapes=[
            pltpu.VMEM((2, 4, 4, NZ, SLOTS, 32, LANES), jnp.float32),
            pltpu.VMEM((2, 4, 2, 256, PANEL), jnp.float32),
            pltpu.VMEM((ROWS, PANEL), jnp.float32),
            pltpu.VMEM((PANELS, 2 * ROWS, PANEL), jnp.bfloat16),
            pltpu.SemaphoreType.DMA,
            pltpu.SemaphoreType.DMA,
            pltpu.SemaphoreType.DMA,
        ],
        compiler_params=pltpu.CompilerParams(vmem_limit_bytes=48 * 2**20),
        cost_estimate=pl.CostEstimate(flops=16 * 10**9, bytes_accessed=40 * 10**6, transcendentals=0),
    )(place, rows, *diagonals, *arrays)


def local(integrals, factor, diag_inverse):
    pair, aux = lax.axis_index("pair"), lax.axis_index("aux")
    x, z, core = pair // 8, (pair // 2) % 4 * 2 + aux // NY, pair % 2
    place = jnp.stack([x, aux % NY, z, core]).astype(jnp.int32)

    column = ring_of_eight(share(spread(factor, pair), pair // 4))
    half = lax.dynamic_slice(diag_inverse[0], (256 * core, 0), (256, PANEL))
    column, half = lax.optimization_barrier((column, half))
    rows, diagonals, gathered = gather(column, half, integrals)
    solved = solve(place, rows, diagonals, gathered)
    result = lax.all_to_all(solved, "aux", 0, 0, tiled=True)
    return result.reshape(1, 8 * ROWS, PANEL)


def solution(mesh):
    in_specs = (P(None, "aux", "pair"), P("aux", "pair"), P("aux", None, None))
    out_specs = P("pair", None, "aux")
    return jax.shard_map(local, mesh=mesh, in_specs=in_specs, out_specs=out_specs, check_vma=False)
```

```python
import jax
import jax.numpy as jnp
from jax import lax
from jax.experimental import pallas as pl
from jax.experimental.pallas import tpu as pltpu
from jax.sharding import PartitionSpec as P


NX, NY, NZ = 4, 4, 8
ALL = ("pair", "aux")
EARLY, LATE = 4, 3
SLOTS = EARLY + LATE
PANELS, PANEL, LANES, ROWS = 8, 512, 128, 80


def device_id(x, y, z, core):
    return ((x * NZ // 2 + z // 2) * 2 + core) * 8 + (z % 2) * NY + y


def shift(value, dx=0, dy=0, dz=0, core=0):
    pairs = [
        (device_id(x, y, z, c), device_id((x + dx) % NX, (y + dy) % NY, (z + dz) % NZ, (c + core) % 2))
        for x in range(NX)
        for y in range(NY)
        for z in range(NZ)
        for c in range(2)
    ]
    return lax.ppermute(value, ALL, pairs)


def ring_of_eight(piece):
    near = [shift(piece, dz=d) for d in (1, -1, 2, -2)]
    one, minus_one, two, minus_two = lax.optimization_barrier(near)
    three, minus_three = shift(two, dz=1), shift(minus_two, dz=-1)
    four = shift(two, dz=2)
    return jnp.stack([piece, one, two, three, four, minus_three, minus_two, minus_one])


def spread(factor, pair):
    halves = factor.reshape(2, 8, 32, LANES)
    halves = jnp.where(pair < 16, halves, halves[::-1]).reshape(16, 32, LANES)
    groups = [[8 * p + a for p in (low, 31 - low) for a in range(8)] for low in range(16)]
    return lax.all_to_all(halves, ALL, 0, 0, axis_index_groups=groups, tiled=True)


def share(both, column):
    least = jnp.minimum(column, 7 - column)
    held = []
    for slot in range(SLOTS):
        paired = (slot + 9) // 2 if slot % 2 else 8 + (slot + 8) // 2
        index = jnp.where(slot < 7 - 2 * least, slot + least + 1, paired)
        held.append(lax.dynamic_index_in_dim(both, index, 0, keepdims=False))
    return jnp.stack(held)


def swap(values):
    return [shift(value, core=1) for value in values]


def gather(column, quarter, integrals):
    early, late = column[:, :EARLY], column[:, EARLY:]
    near = [shift(early, dy=1), shift(early, dy=-1), shift(late, dx=1), shift(late, dx=-1)]
    rows = lax.all_to_all(integrals, "pair", 0, 0, tiled=True)
    neighbour = lax.ppermute(quarter, "aux", [(a, (a + 4) % 8) for a in range(8)])
    up, down, late_up, late_down = lax.optimization_barrier(near)
    ends = [shift(up[:4], dy=1), shift(down[4:], dy=-1)]
    late_ends = [shift(late_up[:4], dx=1), shift(late_down[4:], dx=-1)]
    head = jnp.concatenate([early, up])
    head_up, head_down = shift(head, dx=1), shift(head, dx=-1)
    swapped_head = shift(head, core=1)
    ends, late_ends, swapped_head = lax.optimization_barrier((ends, late_ends, swapped_head))
    tail = jnp.concatenate([down, *ends])
    whole = jnp.concatenate([late, late_up, late_down, *late_ends])
    tail_up, tail_down = shift(tail, dx=1), shift(tail, dx=-1)
    late_up, late_down = shift(whole, dy=1), shift(whole, dy=-1)
    swapped = [swapped_head, *swap([tail, whole, quarter])]
    head_up, swapped = lax.optimization_barrier((head_up, swapped))
    far_up = shift(head_up, dx=1)
    tail_down, late_up, late_down, rows, neighbour = lax.optimization_barrier(
        (tail_down, late_up, late_down, rows, neighbour)
    )
    far_down = shift(tail_down, dx=-1)
    late_far = [shift(late_up[:16], dy=1), shift(late_down[16:], dy=-1)]
    sides = [head_up, tail_up, head_down, tail_down, late_up, late_down, neighbour]
    swapped_sides = swap(sides)
    far, swapped_sides = lax.optimization_barrier(([far_up, far_down, *late_far], swapped_sides))
    swapped_far = swap(far)
    diagonals = [quarter, neighbour, swapped[3], swapped_sides[6]]
    arrays = [head, tail, *sides[:4], *far[:2], *swapped[:2], *swapped_sides[:4], *swapped_far[:2]]
    late_arrays = [whole, *sides[4:6], *far[2:], swapped[2], *swapped_sides[4:6], *swapped_far[2:]]
    return rows, diagonals + arrays + late_arrays


EARLY_LAYOUT = ((0, 0, 2), (0, 2, 2), (1, 0, 2), (1, 2, 2), (2, 0, 2), (2, 2, 2), (3, 0, 2), (3, 2, 2))
LATE_LAYOUT = ((0, 0, 4), (1, 0, 4), (2, 0, 4), (3, 0, 2), (3, 2, 2))


def position(delta):
    delta = lax.rem(delta + 4, 4)
    return jnp.where(delta == 3, 1, jnp.where(delta == 0, 0, delta + 1))


def kernel(*refs):
    place_ref, x_ref = refs[:2]
    diagonals, arrays, late_arrays = refs[2:6], refs[6:22], refs[22:32]
    out_ref, held, inverses, remain, parts, inverse_sem, first_sem, second_sem, late_sem = refs[32:]
    x, y, z, core = (place_ref[i] for i in range(4))

    for other in range(2):
        for z_lo in range(2):
            ref = diagonals[2 * other + z_lo]
            pltpu.make_async_copy(ref, inverses.at[other, z_lo], inverse_sem).start()
    for slots, sem in ((pl.ds(0, 2), first_sem), (pl.ds(2, 2), second_sem)):
        for other in range(2):
            for number, (second, block, count) in enumerate(EARLY_LAYOUT):
                ref = arrays[8 * other + number]
                to = held.at[other, pl.ds(block, count), second, :, slots]
                pltpu.make_async_copy(ref.at[:, :, slots], to, sem).start()
    for other in range(2):
        for number, (second, block, count) in enumerate(LATE_LAYOUT):
            to = held.at[other, second, pl.ds(block, count), :, pl.ds(EARLY, LATE)]
            pltpu.make_async_copy(late_arrays[5 * other + number], to, late_sem).start()
    parts[...] = jnp.zeros_like(parts)
    y_positions = [position(sy - y) for sy in range(NY)]

    def slab(p, slot):
        x_position = position(lax.div(p, 8) - x)
        other = lax.rem(p + core, 2)
        sz = 2 * lax.rem(lax.div(p, 2), 4)
        rows = []
        for z_lo in range(2):
            d = lax.rem(z - sz - z_lo + NZ, NZ)
            rows += [held[other, y_positions[sy], x_position, d, slot] for sy in range(NY)]
        return jnp.concatenate(rows)

    def product(left, loads):
        dims = (((1,), (1,)), ((), ()))
        halves = []
        for half in range(2):
            weight = jnp.concatenate([load(half, side) for load in loads for side in range(2)], axis=1)
            high = weight.astype(jnp.bfloat16)
            low = (weight - high.astype(jnp.float32)).astype(jnp.bfloat16)
            twice = lax.dot_general(left, high, dims, preferred_element_type=jnp.float32)
            once = lax.dot_general(left[:ROWS], low, dims, preferred_element_type=jnp.float32)
            halves.append(twice[:ROWS] + (twice[ROWS:] + once))
        return jnp.concatenate(halves, axis=1)

    def split(value):
        high = value.astype(jnp.bfloat16)
        low = (value - high.astype(jnp.float32)).astype(jnp.bfloat16)
        return jnp.concatenate([high, low], axis=0)

    def block(j, k):
        low_slot = jnp.where(j < 8 - k, jnp.maximum(j - k - 1, 0), 2 * j - 9)
        slot = jnp.where(k < 4, low_slot, 2 * j - 8)

        def load(half, side):
            columns = [4 * k + 2 * side + s for s in range(2)]
            return jnp.concatenate([slab(31 - p if half else p, slot) for p in columns], axis=1)

        return load

    def panel(j, carry):
        for first, slots, sem in ((1, pl.ds(0, 2), first_sem), (3, pl.ds(2, 2), second_sem), (5, pl.ds(EARLY, LATE), late_sem)):

            @pl.when(j == first)
            def _():
                arrived = held.at[:, :, :, :, slots]
                pltpu.make_async_copy(arrived, arrived, sem).wait()

        remain[...] = jnp.concatenate([x_ref[4 * j + s] for s in range(4)], axis=1)

        def update(pair, carry):
            k = 2 * pair
            left = jnp.concatenate([parts[k], parts[k + 1]], axis=1)
            remain[...] -= product(left, [block(j, k), block(j, k + 1)])
            return carry

        lax.fori_loop(0, lax.div(j + 1, 2), update, 0)

        def load(half, side):
            other, z_lo = lax.rem(core + half, 2), lax.rem(z + lax.div(j, 4), 2)
            at = position(lax.rem(j, 4) - y)
            return inverses[other, z_lo, at, :, 256 * side : 256 * (side + 1)]

        solved = product(split(remain[...]), [load])
        out_ref[j] = solved
        parts[j] = split(solved)
        return carry

    pltpu.make_async_copy(inverses, inverses, inverse_sem).wait()
    lax.fori_loop(0, PANELS, panel, 0)


def solve(place, rows, arrays):
    arrays = arrays[:4] + [v.reshape(-1, NZ, *v.shape[1:]) for v in arrays[4:]]
    return pl.pallas_call(
        kernel,
        out_shape=jax.ShapeDtypeStruct((PANELS, ROWS, PANEL), jnp.float32),
        in_specs=[pl.BlockSpec(memory_space=pltpu.SMEM), pl.BlockSpec(memory_space=pltpu.VMEM)]
        + [pl.BlockSpec(memory_space=pl.ANY)] * len(arrays),
        out_specs=pl.BlockSpec(memory_space=pltpu.VMEM),
        scratch_shapes=[
            pltpu.VMEM((2, 4, 4, NZ, SLOTS, 32, LANES), jnp.float32),
            pltpu.VMEM((2, 2, 4, 256, PANEL), jnp.float32),
            pltpu.VMEM((ROWS, PANEL), jnp.float32),
            pltpu.VMEM((PANELS, 2 * ROWS, PANEL), jnp.bfloat16),
        ]
        + [pltpu.SemaphoreType.DMA] * 4,
        compiler_params=pltpu.CompilerParams(vmem_limit_bytes=48 * 2**20),
        cost_estimate=pl.CostEstimate(flops=16 * 10**9, bytes_accessed=40 * 10**6, transcendentals=0),
    )(place, rows, *arrays)


def local(integrals, factor, diag_inverse):
    pair, aux = lax.axis_index("pair"), lax.axis_index("aux")
    x, z, core = pair // 8, (pair // 2) % 4 * 2 + aux // NY, pair % 2
    place = jnp.stack([x, aux % NY, z, core]).astype(jnp.int32)

    half = lax.dynamic_slice(diag_inverse[0], (256 * core, 0), (256, PANEL))
    up, down = shift(half, dy=1), shift(half, dy=-1)
    both, up, down = lax.optimization_barrier((spread(factor, pair), up, down))
    ends = jnp.concatenate([shift(up[:128], dy=1), shift(down[128:], dy=-1)])
    column, ends = lax.optimization_barrier((ring_of_eight(share(both, pair // 4)), ends))
    quarter = jnp.stack([half, up, down, ends])
    rows, arrays = gather(column, quarter, integrals)
    solved = solve(place, rows, arrays)
    result = lax.all_to_all(solved, "aux", 0, 0, tiled=True)
    return result.reshape(1, 8 * ROWS, PANEL)


def solution(mesh):
    in_specs = (P(None, "aux", "pair"), P("aux", "pair"), P("aux", None, None))
    out_specs = P("pair", None, "aux")
    return jax.shard_map(local, mesh=mesh, in_specs=in_specs, out_specs=out_specs, check_vma=False)
```

```python
import jax
import jax.numpy as jnp
from jax import lax
from jax.experimental import pallas as pl
from jax.experimental.pallas import tpu as pltpu
from jax.sharding import PartitionSpec as P


NX, NY, NZ = 4, 4, 8
ALL = ("pair", "aux")
EARLY, LATE = 4, 3
SLOTS = EARLY + LATE
PANELS, PANEL, LANES, ROWS = 8, 512, 128, 80


def device_id(x, y, z, core):
    return ((x * NZ // 2 + z // 2) * 2 + core) * 8 + (z % 2) * NY + y


def shift(value, dx=0, dy=0, dz=0, core=0):
    pairs = [
        (device_id(x, y, z, c), device_id((x + dx) % NX, (y + dy) % NY, (z + dz) % NZ, (c + core) % 2))
        for x in range(NX)
        for y in range(NY)
        for z in range(NZ)
        for c in range(2)
    ]
    return lax.ppermute(value, ALL, pairs)


def ring_of_eight(piece):
    near = [shift(piece, dz=d) for d in (1, -1, 2, -2)]
    one, minus_one, two, minus_two = lax.optimization_barrier(near)
    three, minus_three = shift(two, dz=1), shift(minus_two, dz=-1)
    four = shift(two, dz=2)
    return jnp.stack([piece, one, two, three, four, minus_three, minus_two, minus_one])


def spread(factor, pair):
    halves = factor.reshape(2, 8, 32, LANES)
    halves = jnp.where(pair < 16, halves, halves[::-1]).reshape(16, 32, LANES)
    groups = [[8 * p + a for p in (low, 31 - low) for a in range(8)] for low in range(16)]
    return lax.all_to_all(halves, ALL, 0, 0, axis_index_groups=groups, tiled=True)


def share(both, column):
    least = jnp.minimum(column, 7 - column)
    held = []
    for slot in range(SLOTS):
        paired = (slot + 9) // 2 if slot % 2 else 8 + (slot + 8) // 2
        index = jnp.where(slot < 7 - 2 * least, slot + least + 1, paired)
        held.append(lax.dynamic_index_in_dim(both, index, 0, keepdims=False))
    return jnp.stack(held)


def swap(values):
    return [shift(value, core=1) for value in values]


def gather(column, quarter, integrals):
    early, late = column[:, :EARLY], column[:, EARLY:]
    near = [shift(early, dy=1), shift(early, dy=-1), shift(late, dx=1), shift(late, dx=-1)]
    rows = lax.all_to_all(integrals, "pair", 0, 0, tiled=True)
    neighbour = lax.ppermute(quarter, "aux", [(a, (a + 4) % 8) for a in range(8)])
    up, down, late_up, late_down = lax.optimization_barrier(near)
    ends = [shift(up[:4], dy=1), shift(down[4:], dy=-1)]
    late_ends = [shift(late_up[:4], dx=1), shift(late_down[4:], dx=-1)]
    head = jnp.concatenate([early, up])
    head_up, head_down = shift(head, dx=1), shift(head, dx=-1)
    swapped_head = shift(head, core=1)
    ends, late_ends, swapped_head = lax.optimization_barrier((ends, late_ends, swapped_head))
    tail = jnp.concatenate([down, *ends])
    whole = jnp.concatenate([late, late_up, late_down, *late_ends])
    tail_up, tail_down = shift(tail, dx=1), shift(tail, dx=-1)
    late_up, late_down = shift(whole, dy=1), shift(whole, dy=-1)
    swapped = [swapped_head, *swap([tail, whole, quarter])]
    head_up, swapped = lax.optimization_barrier((head_up, swapped))
    far_up = shift(head_up, dx=1)
    tail_down, late_up, late_down, rows = lax.optimization_barrier((tail_down, late_up, late_down, rows))
    far_down = shift(tail_down, dx=-1)
    late_far = [shift(late_up[:16], dy=1), shift(late_down[16:], dy=-1)]
    sides = [head_up, tail_up, head_down, tail_down, late_up, late_down]
    swapped_sides = swap(sides)
    far, swapped_sides = lax.optimization_barrier(([far_up, far_down, *late_far], swapped_sides))
    swapped_far = swap([*far, neighbour])
    diagonals = [quarter, neighbour, swapped[3], swapped_far[4]]
    arrays = [head, tail, *sides[:4], *far[:2], *swapped[:2], *swapped_sides[:4], *swapped_far[:2]]
    late_arrays = [whole, *sides[4:], *far[2:], swapped[2], *swapped_sides[4:], *swapped_far[2:4]]
    return rows, diagonals + arrays + late_arrays


EARLY_LAYOUT = ((0, 0, 2), (0, 2, 2), (1, 0, 2), (1, 2, 2), (2, 0, 2), (2, 2, 2), (3, 0, 2), (3, 2, 2))
LATE_LAYOUT = ((0, 0, 4), (1, 0, 4), (2, 0, 4), (3, 0, 2), (3, 2, 2))


def position(delta):
    delta = lax.rem(delta + 4, 4)
    return jnp.where(delta == 3, 1, jnp.where(delta == 0, 0, delta + 1))


def kernel(*refs):
    place_ref, x_ref = refs[:2]
    diagonals, arrays, late_arrays = refs[2:6], refs[6:22], refs[22:32]
    out_ref, held, inverses, remain, parts, inverse_sem, first_sem, second_sem, late_sem = refs[32:]
    x, y, z, core = (place_ref[i] for i in range(4))

    for other in range(2):
        for z_lo in range(2):
            ref = diagonals[2 * other + z_lo]
            pltpu.make_async_copy(ref, inverses.at[other, z_lo], inverse_sem).start()
    for slots, sem in ((pl.ds(0, 2), first_sem), (pl.ds(2, 2), second_sem)):
        for other in range(2):
            for number, (second, block, count) in enumerate(EARLY_LAYOUT):
                ref = arrays[8 * other + number]
                to = held.at[other, pl.ds(block, count), second, :, slots]
                pltpu.make_async_copy(ref.at[:, :, slots], to, sem).start()
    for other in range(2):
        for number, (second, block, count) in enumerate(LATE_LAYOUT):
            to = held.at[other, second, pl.ds(block, count), :, pl.ds(EARLY, LATE)]
            pltpu.make_async_copy(late_arrays[5 * other + number], to, late_sem).start()
    parts[...] = jnp.zeros_like(parts)
    y_positions = [position(sy - y) for sy in range(NY)]

    def slab(p, slot):
        x_position = position(lax.div(p, 8) - x)
        other = lax.rem(p + core, 2)
        sz = 2 * lax.rem(lax.div(p, 2), 4)
        rows = []
        for z_lo in range(2):
            d = lax.rem(z - sz - z_lo + NZ, NZ)
            rows += [held[other, y_positions[sy], x_position, d, slot] for sy in range(NY)]
        return jnp.concatenate(rows)

    def product(left, loads):
        dims = (((1,), (1,)), ((), ()))
        halves = []
        for half in range(2):
            weight = jnp.concatenate([load(half, side) for load in loads for side in range(2)], axis=1)
            high = weight.astype(jnp.bfloat16)
            low = (weight - high.astype(jnp.float32)).astype(jnp.bfloat16)
            twice = lax.dot_general(left, high, dims, preferred_element_type=jnp.float32)
            once = lax.dot_general(left[:ROWS], low, dims, preferred_element_type=jnp.float32)
            halves.append(twice[:ROWS] + (twice[ROWS:] + once))
        return jnp.concatenate(halves, axis=1)

    def split(value):
        high = value.astype(jnp.bfloat16)
        low = (value - high.astype(jnp.float32)).astype(jnp.bfloat16)
        return jnp.concatenate([high, low], axis=0)

    def block(j, k):
        low_slot = jnp.where(j < 8 - k, jnp.maximum(j - k - 1, 0), 2 * j - 9)
        slot = jnp.where(k < 4, low_slot, 2 * j - 8)

        def load(half, side):
            columns = [4 * k + 2 * side + s for s in range(2)]
            return jnp.concatenate([slab(31 - p if half else p, slot) for p in columns], axis=1)

        return load

    def panel(j, carry):
        for first, slots, sem in ((1, pl.ds(0, 2), first_sem), (3, pl.ds(2, 2), second_sem), (5, pl.ds(EARLY, LATE), late_sem)):

            @pl.when(j == first)
            def _():
                arrived = held.at[:, :, :, :, slots]
                pltpu.make_async_copy(arrived, arrived, sem).wait()

        remain[...] = jnp.concatenate([x_ref[4 * j + s] for s in range(4)], axis=1)

        def update(pair, carry):
            k = 2 * pair
            left = jnp.concatenate([parts[k], parts[k + 1]], axis=1)
            remain[...] -= product(left, [block(j, k), block(j, k + 1)])
            return carry

        lax.fori_loop(0, lax.div(j + 1, 2), update, 0)

        def load(half, side):
            other, z_lo = lax.rem(core + half, 2), lax.rem(z + lax.div(j, 4), 2)
            at = position(lax.rem(j, 4) - y)
            return inverses[other, z_lo, at, :, 256 * side : 256 * (side + 1)]

        solved = product(split(remain[...]), [load])
        out_ref[j] = solved
        parts[j] = split(solved)
        return carry

    pltpu.make_async_copy(inverses, inverses, inverse_sem).wait()
    lax.fori_loop(0, PANELS, panel, 0)


def solve(place, rows, arrays):
    arrays = arrays[:4] + [v.reshape(-1, NZ, *v.shape[1:]) for v in arrays[4:]]
    return pl.pallas_call(
        kernel,
        out_shape=jax.ShapeDtypeStruct((PANELS, ROWS, PANEL), jnp.float32),
        in_specs=[pl.BlockSpec(memory_space=pltpu.SMEM), pl.BlockSpec(memory_space=pltpu.VMEM)]
        + [pl.BlockSpec(memory_space=pl.ANY)] * len(arrays),
        out_specs=pl.BlockSpec(memory_space=pltpu.VMEM),
        scratch_shapes=[
            pltpu.VMEM((2, 4, 4, NZ, SLOTS, 32, LANES), jnp.float32),
            pltpu.VMEM((2, 2, 4, 256, PANEL), jnp.float32),
            pltpu.VMEM((ROWS, PANEL), jnp.float32),
            pltpu.VMEM((PANELS, 2 * ROWS, PANEL), jnp.bfloat16),
        ]
        + [pltpu.SemaphoreType.DMA] * 4,
        compiler_params=pltpu.CompilerParams(vmem_limit_bytes=48 * 2**20),
        cost_estimate=pl.CostEstimate(flops=16 * 10**9, bytes_accessed=40 * 10**6, transcendentals=0),
    )(place, rows, *arrays)


def local(integrals, factor, diag_inverse):
    pair, aux = lax.axis_index("pair"), lax.axis_index("aux")
    x, z, core = pair // 8, (pair // 2) % 4 * 2 + aux // NY, pair % 2
    place = jnp.stack([x, aux % NY, z, core]).astype(jnp.int32)

    half = lax.dynamic_slice(diag_inverse[0], (256 * core, 0), (256, PANEL))
    up, down = shift(half, dy=1), shift(half, dy=-1)
    both, up, down = lax.optimization_barrier((spread(factor, pair), up, down))
    ends = jnp.concatenate([shift(up[:128], dy=1), shift(down[128:], dy=-1)])
    column, ends = lax.optimization_barrier((ring_of_eight(share(both, pair // 4)), ends))
    quarter = jnp.stack([half, up, down, ends])
    rows, arrays = gather(column, quarter, integrals)
    solved = solve(place, rows, arrays)
    result = lax.all_to_all(solved, "aux", 0, 0, tiled=True)
    return result.reshape(1, 8 * ROWS, PANEL)


def solution(mesh):
    in_specs = (P(None, "aux", "pair"), P("aux", "pair"), P("aux", None, None))
    out_specs = P("pair", None, "aux")
    return jax.shard_map(local, mesh=mesh, in_specs=in_specs, out_specs=out_specs, check_vma=False)
```

```python
import jax
import jax.numpy as jnp
from jax import lax
from jax.experimental import pallas as pl
from jax.experimental.pallas import tpu as pltpu
from jax.sharding import PartitionSpec as P


NX, NY, NZ = 4, 4, 8
ALL = ("pair", "aux")
EARLY, LATE = 4, 3
SLOTS = EARLY + LATE
PANELS, PANEL, LANES, ROWS = 8, 512, 128, 80


def device_id(x, y, z, core):
    return ((x * NZ // 2 + z // 2) * 2 + core) * 8 + (z % 2) * NY + y


def shift(value, dx=0, dy=0, dz=0, core=0):
    pairs = [
        (device_id(x, y, z, c), device_id((x + dx) % NX, (y + dy) % NY, (z + dz) % NZ, (c + core) % 2))
        for x in range(NX)
        for y in range(NY)
        for z in range(NZ)
        for c in range(2)
    ]
    return lax.ppermute(value, ALL, pairs)


def ring_of_eight(piece):
    near = [shift(piece, dz=d) for d in (1, -1, 2, -2)]
    one, minus_one, two, minus_two = lax.optimization_barrier(near)
    three, minus_three = shift(two, dz=1), shift(minus_two, dz=-1)
    four = shift(two, dz=2)
    return jnp.stack([piece, one, two, three, four, minus_three, minus_two, minus_one])


def spread(factor, pair):
    halves = factor.reshape(2, 8, 32, LANES)
    halves = jnp.where(pair < 16, halves, halves[::-1]).reshape(16, 32, LANES)
    groups = [[8 * p + a for p in (low, 31 - low) for a in range(8)] for low in range(16)]
    return lax.all_to_all(halves, ALL, 0, 0, axis_index_groups=groups, tiled=True)


def share(both, column):
    least = jnp.minimum(column, 7 - column)
    held = []
    for slot in range(SLOTS):
        paired = (slot + 9) // 2 if slot % 2 else 8 + (slot + 8) // 2
        index = jnp.where(slot < 7 - 2 * least, slot + least + 1, paired)
        held.append(lax.dynamic_index_in_dim(both, index, 0, keepdims=False))
    return jnp.stack(held)


def swap(values):
    return [shift(value, core=1) for value in values]


def gather(column, quarter, integrals):
    early, late = column[:, :EARLY], column[:, EARLY:]
    near = [shift(early, dy=1), shift(early, dy=-1), shift(late, dx=1), shift(late, dx=-1)]
    rows = lax.all_to_all(integrals, "pair", 0, 0, tiled=True)
    neighbour = lax.ppermute(quarter, "aux", [(a, (a + 4) % 8) for a in range(8)])
    up, down, late_up, late_down = lax.optimization_barrier(near)
    ends = [shift(up[:4], dy=1), shift(down[4:], dy=-1)]
    late_ends = [shift(late_up[:4], dx=1), shift(late_down[4:], dx=-1)]
    head = jnp.concatenate([early, up])
    head_up, head_down = shift(head, dx=1), shift(head, dx=-1)
    swapped_head = shift(head, core=1)
    ends, late_ends, swapped_head = lax.optimization_barrier((ends, late_ends, swapped_head))
    tail = jnp.concatenate([down, *ends])
    whole = jnp.concatenate([late, late_up, late_down, *late_ends])
    tail_up, tail_down = shift(tail, dx=1), shift(tail, dx=-1)
    late_up, late_down = shift(whole, dy=1), shift(whole, dy=-1)
    swapped = [swapped_head, *swap([tail, whole, quarter])]
    head_up, swapped = lax.optimization_barrier((head_up, swapped))
    far_up = shift(head_up, dx=1)
    tail_down, late_up, late_down, rows = lax.optimization_barrier((tail_down, late_up, late_down, rows))
    far_down = shift(tail_down, dx=-1)
    late_far = [shift(late_up[:16], dy=1), shift(late_down[16:], dy=-1)]
    sides = [head_up, tail_up, head_down, tail_down, late_up, late_down]
    swapped_sides = swap(sides)
    far, swapped_sides = lax.optimization_barrier(([far_up, far_down, *late_far], swapped_sides))
    swapped_far = swap([*far, neighbour])
    diagonals = [quarter, neighbour, swapped[3], swapped_far[4]]
    arrays = [head, tail, *sides[:4], *far[:2], *swapped[:2], *swapped_sides[:4], *swapped_far[:2]]
    late_arrays = [whole, *sides[4:], *far[2:], swapped[2], *swapped_sides[4:], *swapped_far[2:4]]
    return rows, diagonals + arrays + late_arrays


EARLY_LAYOUT = ((0, 0, 2), (0, 2, 2), (1, 0, 2), (1, 2, 2), (2, 0, 2), (2, 2, 2), (3, 0, 2), (3, 2, 2))
LATE_LAYOUT = ((0, 0, 4), (1, 0, 4), (2, 0, 4), (3, 0, 2), (3, 2, 2))


def position(delta):
    delta = lax.rem(delta + 4, 4)
    return jnp.where(delta == 3, 1, jnp.where(delta == 0, 0, delta + 1))


def kernel(*refs):
    place_ref, x_ref = refs[:2]
    diagonals, arrays, late_arrays = refs[2:6], refs[6:22], refs[22:32]
    out_ref, held, inverses, remain, parts, firsts, inverse_sem, first_sem, second_sem, late_sem = refs[32:]
    x, y, z, core = (place_ref[i] for i in range(4))

    for other in range(2):
        for z_lo in range(2):
            ref = diagonals[2 * other + z_lo]
            pltpu.make_async_copy(ref, inverses.at[other, z_lo], inverse_sem).start()
    for slots, sem in ((pl.ds(0, 2), first_sem), (pl.ds(2, 2), second_sem)):
        for other in range(2):
            for number, (second, block, count) in enumerate(EARLY_LAYOUT):
                ref = arrays[8 * other + number]
                to = held.at[other, pl.ds(block, count), second, :, slots]
                pltpu.make_async_copy(ref.at[:, :, slots], to, sem).start()
    for other in range(2):
        for number, (second, block, count) in enumerate(LATE_LAYOUT):
            to = held.at[other, second, pl.ds(block, count), :, pl.ds(EARLY, LATE)]
            pltpu.make_async_copy(late_arrays[5 * other + number], to, late_sem).start()
    parts[...] = jnp.zeros_like(parts)
    y_offsets = [position(sy - y) * (4 * NZ * SLOTS) for sy in range(NY)]
    flat = held.reshape(256 * SLOTS, 32, LANES)

    @pl.loop(0, 32)
    def _(p):
        base = (lax.rem(p + core, 2) * 16 + position(lax.div(p, 8) - x)) * NZ
        for z_lo in range(2):
            d = lax.rem(z - 2 * lax.rem(lax.div(p, 2), 4) - z_lo + NZ, NZ)
            firsts[2 * p + z_lo] = (base + d) * SLOTS

    def slab(p, slot):
        rows = []
        for z_lo in range(2):
            at = firsts[2 * p + z_lo] + slot
            rows += [flat[at + y_offsets[sy]] for sy in range(NY)]
        return jnp.concatenate(rows)

    def product(right, load):
        halves = []
        for half in range(2):
            weight = jnp.concatenate([load(half, side) for side in range(2)], axis=1)
            high = weight.astype(jnp.bfloat16)
            low = (weight - high.astype(jnp.float32)).astype(jnp.bfloat16)
            both = jnp.dot(jnp.concatenate([high, low]), right, preferred_element_type=jnp.float32)
            halves.append(both[:256, :ROWS] + (both[:256, LANES : LANES + ROWS] + both[256:, :ROWS]))
        return jnp.concatenate(halves)

    def split(value, to):
        high = value.astype(jnp.bfloat16)
        to[:, :ROWS] = high
        to[:, LANES : LANES + ROWS] = (value - high.astype(jnp.float32)).astype(jnp.bfloat16)

    def block(j, k):
        low_slot = jnp.where(j < 8 - k, j - k - 1, 2 * j - 9)
        slot = jnp.where(k < 4, low_slot, 2 * j - 8)

        def load(half, side):
            columns = [4 * k + 2 * side + s for s in range(2)]
            return jnp.concatenate([slab(31 - p if half else p, slot) for p in columns], axis=1)

        return load

    def panel(j, carry):
        for first, slots, sem in ((1, pl.ds(0, 2), first_sem), (3, pl.ds(2, 2), second_sem), (5, pl.ds(EARLY, LATE), late_sem)):

            @pl.when(j == first)
            def _():
                arrived = held.at[:, :, :, :, slots]
                pltpu.make_async_copy(arrived, arrived, sem).wait()

        remain[...] = jnp.concatenate([x_ref[4 * j + s].T for s in range(4)])

        def update(k, carry):
            remain[...] -= product(parts[k], block(j, k))
            return carry

        lax.fori_loop(0, j, update, 0)

        def load(half, side):
            other, z_lo = lax.rem(core + half, 2), lax.rem(z + lax.div(j, 4), 2)
            at = position(lax.rem(j, 4) - y)
            return inverses[other, z_lo, at, :, 256 * side : 256 * (side + 1)]

        split(remain[...], parts.at[j])
        solved = product(parts[j], load)
        out_ref[j] = solved.T
        split(solved, parts.at[j])
        return carry

    pltpu.make_async_copy(inverses, inverses, inverse_sem).wait()
    lax.fori_loop(0, PANELS, panel, 0)


def solve(place, rows, arrays):
    arrays = arrays[:4] + [v.reshape(-1, NZ, *v.shape[1:]) for v in arrays[4:]]
    return pl.pallas_call(
        kernel,
        out_shape=jax.ShapeDtypeStruct((PANELS, ROWS, PANEL), jnp.float32),
        in_specs=[pl.BlockSpec(memory_space=pltpu.SMEM), pl.BlockSpec(memory_space=pltpu.VMEM)]
        + [pl.BlockSpec(memory_space=pl.ANY)] * len(arrays),
        out_specs=pl.BlockSpec(memory_space=pltpu.VMEM),
        scratch_shapes=[
            pltpu.VMEM((2, 4, 4, NZ, SLOTS, 32, LANES), jnp.float32),
            pltpu.VMEM((2, 2, 4, 256, PANEL), jnp.float32),
            pltpu.VMEM((PANEL, ROWS), jnp.float32),
            pltpu.VMEM((PANELS, PANEL, 2 * LANES), jnp.bfloat16),
            pltpu.SMEM((64,), jnp.int32),
        ]
        + [pltpu.SemaphoreType.DMA] * 4,
        compiler_params=pltpu.CompilerParams(vmem_limit_bytes=48 * 2**20),
        cost_estimate=pl.CostEstimate(flops=16 * 10**9, bytes_accessed=40 * 10**6, transcendentals=0),
    )(place, rows, *arrays)


def local(integrals, factor, diag_inverse):
    pair, aux = lax.axis_index("pair"), lax.axis_index("aux")
    x, z, core = pair // 8, (pair // 2) % 4 * 2 + aux // NY, pair % 2
    place = jnp.stack([x, aux % NY, z, core]).astype(jnp.int32)

    half = lax.dynamic_slice(diag_inverse[0], (256 * core, 0), (256, PANEL))
    up, down = shift(half, dy=1), shift(half, dy=-1)
    both, up, down = lax.optimization_barrier((spread(factor, pair), up, down))
    ends = jnp.concatenate([shift(up[:128], dy=1), shift(down[128:], dy=-1)])
    column, ends = lax.optimization_barrier((ring_of_eight(share(both, pair // 4)), ends))
    quarter = jnp.stack([half, up, down, ends])
    rows, arrays = gather(column, quarter, integrals)
    solved = solve(place, rows, arrays)
    result = lax.all_to_all(solved, "aux", 0, 0, tiled=True)
    return result.reshape(1, 8 * ROWS, PANEL)


def solution(mesh):
    in_specs = (P(None, "aux", "pair"), P("aux", "pair"), P("aux", None, None))
    out_specs = P("pair", None, "aux")
    return jax.shard_map(local, mesh=mesh, in_specs=in_specs, out_specs=out_specs, check_vma=False)
```

```python
import jax
import jax.numpy as jnp
from jax import lax
from jax.experimental import pallas as pl
from jax.experimental.pallas import tpu as pltpu
from jax.sharding import PartitionSpec as P


NX, NY, NZ = 4, 4, 8
ALL = ("pair", "aux")
EARLY, LATE = 4, 3
SLOTS = EARLY + LATE
PANELS, PANEL, LANES, ROWS = 8, 512, 128, 80


def device_id(x, y, z, core):
    return ((x * NZ // 2 + z // 2) * 2 + core) * 8 + (z % 2) * NY + y


def shift(value, dx=0, dy=0, dz=0, core=0):
    pairs = [
        (device_id(x, y, z, c), device_id((x + dx) % NX, (y + dy) % NY, (z + dz) % NZ, (c + core) % 2))
        for x in range(NX)
        for y in range(NY)
        for z in range(NZ)
        for c in range(2)
    ]
    return lax.ppermute(value, ALL, pairs)


def ring_of_eight(piece):
    near = [shift(piece, dz=d) for d in (1, -1, 2, -2)]
    one, minus_one, two, minus_two = lax.optimization_barrier(near)
    three, minus_three = shift(two, dz=1), shift(minus_two, dz=-1)
    four = shift(two, dz=2)
    return jnp.stack([piece, one, two, three, four, minus_three, minus_two, minus_one])


def spread(factor, pair):
    halves = factor.reshape(2, 8, 32, LANES)
    halves = jnp.where(pair < 16, halves, halves[::-1]).reshape(16, 32, LANES)
    groups = [[8 * p + a for p in (low, 31 - low) for a in range(8)] for low in range(16)]
    return lax.all_to_all(halves, ALL, 0, 0, axis_index_groups=groups, tiled=True)


def share(both, column):
    least = jnp.minimum(column, 7 - column)
    held = []
    for slot in range(SLOTS):
        paired = (slot + 9) // 2 if slot % 2 else 8 + (slot + 8) // 2
        index = jnp.where(slot < 7 - 2 * least, slot + least + 1, paired)
        held.append(lax.dynamic_index_in_dim(both, index, 0, keepdims=False))
    return jnp.stack(held)


def swap(values):
    return [shift(value, core=1) for value in values]


def gather(column, quarter, integrals):
    early, late = column[:, :EARLY], column[:, EARLY:]
    near = [shift(early, dy=1), shift(early, dy=-1), shift(late, dx=1), shift(late, dx=-1)]
    rows = lax.all_to_all(integrals, "pair", 0, 0, tiled=True)
    neighbour = lax.ppermute(quarter, "aux", [(a, (a + 4) % 8) for a in range(8)])
    up, down, late_up, late_down = lax.optimization_barrier(near)
    ends = [shift(up[:4], dy=1), shift(down[4:], dy=-1)]
    late_ends = [shift(late_up[:4], dx=1), shift(late_down[4:], dx=-1)]
    head = jnp.concatenate([early, up])
    head_up, head_down = shift(head, dx=1), shift(head, dx=-1)
    swapped_head = shift(head, core=1)
    ends, late_ends, swapped_head = lax.optimization_barrier((ends, late_ends, swapped_head))
    tail = jnp.concatenate([down, *ends])
    whole = jnp.concatenate([late, late_up, late_down, *late_ends])
    tail_up, tail_down = shift(tail, dx=1), shift(tail, dx=-1)
    late_up, late_down = shift(whole, dy=1), shift(whole, dy=-1)
    swapped = [swapped_head, *swap([tail, whole, quarter])]
    head_up, swapped = lax.optimization_barrier((head_up, swapped))
    far_up = shift(head_up, dx=1)
    swapped_up = shift(head_up, core=1)
    late_up, late_down, rows, swapped_up = lax.optimization_barrier((late_up, late_down, rows, swapped_up))
    far_down = shift(tail_down, dx=-1)
    late_far = [shift(late_up[:16], dy=1), shift(late_down[16:], dy=-1)]
    sides = [head_up, tail_up, head_down, tail_down, late_up, late_down]
    swapped_sides = [swapped_up, *swap(sides[1:])]
    far, swapped_sides = lax.optimization_barrier(([far_up, far_down, *late_far], swapped_sides))
    swapped_far = swap([*far, neighbour])
    diagonals = [quarter, neighbour, swapped[3], swapped_far[4]]
    arrays = [head, tail, *sides[:4], *far[:2], *swapped[:2], *swapped_sides[:4], *swapped_far[:2]]
    late_arrays = [whole, *sides[4:], *far[2:], swapped[2], *swapped_sides[4:], *swapped_far[2:4]]
    return rows, diagonals + arrays + late_arrays


EARLY_LAYOUT = ((0, 0, 2), (0, 2, 2), (1, 0, 2), (1, 2, 2), (2, 0, 2), (2, 2, 2), (3, 0, 2), (3, 2, 2))
LATE_LAYOUT = ((0, 0, 4), (1, 0, 4), (2, 0, 4), (3, 0, 2), (3, 2, 2))


def position(delta):
    delta = lax.rem(delta + 4, 4)
    return jnp.where(delta == 3, 1, jnp.where(delta == 0, 0, delta + 1))


def kernel(*refs):
    place_ref, x_ref = refs[:2]
    diagonals, arrays, late_arrays = refs[2:6], refs[6:22], refs[22:32]
    out_ref, held, inverses, remain, parts, firsts, inverse_sem, first_sem, second_sem, late_sem = refs[32:]
    x, y, z, core = (place_ref[i] for i in range(4))

    for other in range(2):
        for z_lo in range(2):
            ref = diagonals[2 * other + z_lo]
            pltpu.make_async_copy(ref, inverses.at[other, z_lo], inverse_sem).start()
    for slots, sem in ((pl.ds(0, 2), first_sem), (pl.ds(2, 2), second_sem)):
        for other in range(2):
            for number, (second, block, count) in enumerate(EARLY_LAYOUT):
                ref = arrays[8 * other + number]
                to = held.at[other, pl.ds(block, count), second, :, slots]
                pltpu.make_async_copy(ref.at[:, :, slots], to, sem).start()
    for other in range(2):
        for number, (second, block, count) in enumerate(LATE_LAYOUT):
            to = held.at[other, second, pl.ds(block, count), :, pl.ds(EARLY, LATE)]
            pltpu.make_async_copy(late_arrays[5 * other + number], to, late_sem).start()
    parts[...] = jnp.zeros_like(parts)
    y_offsets = [position(sy - y) * (4 * NZ * SLOTS) for sy in range(NY)]
    flat = held.reshape(256 * SLOTS, 32, LANES)

    @pl.loop(0, 32)
    def _(p):
        base = (lax.rem(p + core, 2) * 16 + position(lax.div(p, 8) - x)) * NZ
        for z_lo in range(2):
            d = lax.rem(z - 2 * lax.rem(lax.div(p, 2), 4) - z_lo + NZ, NZ)
            firsts[2 * p + z_lo] = (base + d) * SLOTS

    def slab(p, slot):
        rows = []
        for z_lo in range(2):
            at = firsts[2 * p + z_lo] + slot
            rows += [flat[at + y_offsets[sy]] for sy in range(NY)]
        return jnp.concatenate(rows)

    def product(right, load):
        halves = []
        for half in range(2):
            weight = jnp.concatenate([load(half, side) for side in range(2)], axis=1)
            high = weight.astype(jnp.bfloat16)
            low = (weight - high.astype(jnp.float32)).astype(jnp.bfloat16)
            both = jnp.dot(jnp.concatenate([high, low]), right, preferred_element_type=jnp.float32)
            halves.append(both[:256, :ROWS] + (both[:256, LANES : LANES + ROWS] + both[256:, :ROWS]))
        return jnp.concatenate(halves)

    def split(value, to):
        high = value.astype(jnp.bfloat16)
        to[:, :ROWS] = high
        to[:, LANES : LANES + ROWS] = (value - high.astype(jnp.float32)).astype(jnp.bfloat16)

    def block(j, k):
        low_slot = jnp.where(j < 8 - k, j - k - 1, 2 * j - 9)
        slot = jnp.where(k < 4, low_slot, 2 * j - 8)

        def load(half, side):
            columns = [4 * k + 2 * side + s for s in range(2)]
            return jnp.concatenate([slab(31 - p if half else p, slot) for p in columns], axis=1)

        return load

    def panel(j, carry):
        for first, slots, sem in ((1, pl.ds(0, 2), first_sem), (3, pl.ds(2, 2), second_sem), (5, pl.ds(EARLY, LATE), late_sem)):

            @pl.when(j == first)
            def _():
                arrived = held.at[:, :, :, :, slots]
                pltpu.make_async_copy(arrived, arrived, sem).wait()

        remain[...] = jnp.concatenate([x_ref[4 * j + s].T for s in range(4)])

        def update(k, carry):
            remain[...] -= product(parts[k], block(j, k))
            return carry

        lax.fori_loop(0, j, update, 0)

        def load(half, side):
            other, z_lo = lax.rem(core + half, 2), lax.rem(z + lax.div(j, 4), 2)
            at = position(lax.rem(j, 4) - y)
            return inverses[other, z_lo, at, :, 256 * side : 256 * (side + 1)]

        split(remain[...], parts.at[j])
        solved = product(parts[j], load)
        out_ref[j] = solved.T
        split(solved, parts.at[j])
        return carry

    pltpu.make_async_copy(inverses, inverses, inverse_sem).wait()
    lax.fori_loop(0, PANELS, panel, 0)


def solve(place, rows, arrays):
    arrays = arrays[:4] + [v.reshape(-1, NZ, *v.shape[1:]) for v in arrays[4:]]
    return pl.pallas_call(
        kernel,
        out_shape=jax.ShapeDtypeStruct((PANELS, ROWS, PANEL), jnp.float32),
        in_specs=[pl.BlockSpec(memory_space=pltpu.SMEM), pl.BlockSpec(memory_space=pltpu.VMEM)]
        + [pl.BlockSpec(memory_space=pl.ANY)] * len(arrays),
        out_specs=pl.BlockSpec(memory_space=pltpu.VMEM),
        scratch_shapes=[
            pltpu.VMEM((2, 4, 4, NZ, SLOTS, 32, LANES), jnp.float32),
            pltpu.VMEM((2, 2, 4, 256, PANEL), jnp.float32),
            pltpu.VMEM((PANEL, ROWS), jnp.float32),
            pltpu.VMEM((PANELS, PANEL, 2 * LANES), jnp.bfloat16),
            pltpu.SMEM((64,), jnp.int32),
        ]
        + [pltpu.SemaphoreType.DMA] * 4,
        compiler_params=pltpu.CompilerParams(vmem_limit_bytes=48 * 2**20),
        cost_estimate=pl.CostEstimate(flops=16 * 10**9, bytes_accessed=40 * 10**6, transcendentals=0),
    )(place, rows, *arrays)


def local(integrals, factor, diag_inverse):
    pair, aux = lax.axis_index("pair"), lax.axis_index("aux")
    x, z, core = pair // 8, (pair // 2) % 4 * 2 + aux // NY, pair % 2
    place = jnp.stack([x, aux % NY, z, core]).astype(jnp.int32)

    half = lax.dynamic_slice(diag_inverse[0], (256 * core, 0), (256, PANEL))
    up, down = shift(half, dy=1), shift(half, dy=-1)
    both, up, down = lax.optimization_barrier((spread(factor, pair), up, down))
    ends = jnp.concatenate([shift(up[:128], dy=1), shift(down[128:], dy=-1)])
    column, ends = lax.optimization_barrier((ring_of_eight(share(both, pair // 4)), ends))
    quarter = jnp.stack([half, up, down, ends])
    rows, arrays = gather(column, quarter, integrals)
    solved = solve(place, rows, arrays)
    result = lax.all_to_all(solved, "aux", 0, 0, tiled=True)
    return result.reshape(1, 8 * ROWS, PANEL)


def solution(mesh):
    in_specs = (P(None, "aux", "pair"), P("aux", "pair"), P("aux", None, None))
    out_specs = P("pair", None, "aux")
    return jax.shard_map(local, mesh=mesh, in_specs=in_specs, out_specs=out_specs, check_vma=False)
```
